128 devices in a mesh: gx: 8 (over y, z_lo), gy: 4 (over x), gz: 4 (over z_hi, core).
Axes of the slice: x: 4, y: 4, z: 4 (z_hi: 2, z_lo: 2; z = z_hi * 2 + z_lo), core: 2. Of those that a mesh axis runs over, the one named last changes fastest.
Arguments:
- targets: float32 [512, 512, 512], P('gx', 'gy', 'gz'), may hold values from -6 to 6
- basis_first: float32 [512, 512], replicated, may hold values from -0.25 to 0.25
- basis_second: float32 [512, 512], replicated, may hold values from -0.25 to 0.25
- basis_third: float32 [512, 512], replicated, may hold values from -0.25 to 0.25
- eigen_first: float32 [512], replicated, may hold values from 0.1 to 1
- eigen_second: float32 [512], replicated, may hold values from 0.1 to 1
- eigen_third: float32 [512], replicated, may hold values from 0.1 to 1
- noise: float32 [1], replicated, may hold values from 0.5 to 1
Outputs:
- weights: float32 [512, 512, 512], P('gx', 'gy', 'gz')
The draws below stay inside these ranges and needn't reach their ends.
All inputs are finite; a program needn't handle non-finite values.
Results may differ from the reference program's by a relative error of at most 0.000071.
Values sent between devices are 32-bit elements; how exact they have to be, the bound alone decides.
A program may use at most 64 MiB of HBM per device.

```python
import math
import jax
import jax.numpy as jnp
from jax import lax

N1 = 512
N2 = 512
N3 = 512


def steps_of(own_key, shape, shards, smallest, largest):
    def one(position, shards_of):
        heights = jax.random.uniform(jax.random.fold_in(jax.random.fold_in(own_key, 6), position), (shards_of,), jnp.float32, smallest / len(shards), largest / len(shards))
        return jnp.repeat(jnp.exp(heights), shape[position] // shards_of).reshape((-1,) + (1,) * (len(shape) - position - 1))

    loudness = one(*shards[0])
    for cut in shards[1:]:
        loudness = loudness * one(*cut)
    return loudness


def normal_values(stream_key, extent, spread, reach, split=(), kind=jnp.bfloat16):
    values = spread * jax.random.normal(stream_key, extent, jnp.float32)
    if split:
        values = values * steps_of(stream_key, extent, split, -0.22, 0.18)
    return jnp.clip(values, -reach, reach).astype(kind)


def setup_inputs(seed: int = 0) -> dict:
    streams_of = jax.random.split(jax.random.key(seed), 9)
    return {
        "targets": normal_values(streams_of[0], (N1, N2, N3), 1.0, 6.0, ((0, 8), (1, 4), (2, 4)), jnp.float32),
        "basis_first": normal_values(streams_of[1], (N1, N1), N1 ** -0.5, 0.25, (), jnp.float32),
        "basis_second": normal_values(streams_of[2], (N2, N2), N2 ** -0.5, 0.25, (), jnp.float32),
        "basis_third": normal_values(streams_of[3], (N3, N3), N3 ** -0.5, 0.25, (), jnp.float32),
        "eigen_first": jnp.clip(jnp.exp(jax.random.uniform(streams_of[4], (N1,), jnp.float32, math.log(0.1), math.log(1.0))), 0.1, 1.0),
        "eigen_second": jnp.clip(jnp.exp(jax.random.uniform(streams_of[5], (N2,), jnp.float32, math.log(0.1), math.log(1.0))), 0.1, 1.0),
        "eigen_third": jnp.clip(jnp.exp(jax.random.uniform(streams_of[6], (N3,), jnp.float32, math.log(0.1), math.log(1.0))), 0.1, 1.0),
        "noise": jnp.clip(jnp.exp(jax.random.uniform(streams_of[7], (1,), jnp.float32, math.log(0.5), math.log(1.0))), 0.5, 1.0),
    }


def reference(targets, basis_first, basis_second, basis_third, eigen_first, eigen_second, eigen_third, noise):
    high = lax.Precision.HIGHEST
    rotated = jnp.einsum('ijk,ia->ajk', targets, basis_first, precision=high)
    rotated = jnp.einsum('ajk,jb->abk', rotated, basis_second, precision=high)
    rotated = jnp.einsum('abk,kc->abc', rotated, basis_third, precision=high)
    spectrum = eigen_first[:, None, None] * eigen_second[None, :, None] * eigen_third[None, None, :] + noise[0]
    scaled = rotated / spectrum
    result = jnp.einsum('abc,kc->abk', scaled, basis_third, precision=high)
    result = jnp.einsum('abk,jb->ajk', result, basis_second, precision=high)
    result = jnp.einsum('ajk,ia->ijk', result, basis_first, precision=high)
    return result
```

```python
import functools

import jax
import jax.numpy as jnp
from jax import lax
from jax.experimental import pallas as pl
from jax.experimental.pallas import tpu as pltpu
from jax.sharding import PartitionSpec as P

MESH = pl.DeviceIdType.MESH
BF = jnp.bfloat16
F32 = jnp.float32
STEPS = 4
DEPTH = 512


def halves(value):
    high = value.astype(BF)
    return high, (value - high.astype(F32)).astype(BF)


def kernel(
    t_ref, b1_ref, b2_ref, b3_ref, e1_ref, e2_ref, e3_ref, noise_ref, o_ref,
    re1, se2, re2, se3, rq1, sq2, rq2, sq3, r3, s3,
    re3p, se2p, re2p, se1p, rq3p, sq2p, rq2p, sq1p,
    b1f, b2f, b3f, b3c, b3tc, b2l, b2tl, b1l, b1tl, lhs, rhs, e1b,
    base_sem, send, in_e1, in_q1, in_e2, in_q2, in_mid, in_e3p, in_q3p, in_e2p, in_q2p, in_out,
):
    w, x, q = lax.axis_index("gx"), lax.axis_index("gy"), lax.axis_index("gz")
    y, z, core = w // 2, (q // 2) * 2 + w % 2, q % 2
    beta = w * 4 + q

    def far(n):
        pair = n // 2
        y2 = (y + pair % 4) % 4
        z2 = (z + pair % 4 + pair // 4) % 4
        c2 = (core + n % 2) % 2
        return y2 * 2 + z2 % 2, (z2 // 2) * 2 + c2

    def push(src, dst, sem, arrival, where):
        pltpu.make_async_remote_copy(
            src_ref=src, dst_ref=dst, send_sem=send.at[sem], recv_sem=arrival,
            device_id=where, device_id_type=MESH,
        ).start()

    def await_bytes(ref, sem):
        pltpu.make_async_copy(ref, ref, sem).wait()

    loads = [
        pltpu.make_async_copy(ref, buf, base_sem.at[n])
        for n, (ref, buf) in enumerate(((b3_ref, b3f), (b2_ref, b2f), (b1_ref, b1f)))
    ]
    for load in loads:
        load.start()

    barrier = pltpu.get_barrier_semaphore()

    def greet(n, _):
        w2, q2 = far(n)
        pl.semaphore_signal(barrier, inc=1, device_id=(w2, x, q2), device_id_type=MESH)
        return _

    for d in (1, 2, 3):
        pl.semaphore_signal(barrier, inc=1, device_id=(w, (x + d) % 4, q), device_id_type=MESH)
    lax.fori_loop(1, 32, greet, 0)
    pl.semaphore_wait(barrier, 34)

    def first(s, _):
        two = pl.ds(s * 2, 2)
        for d in (2, 1, 3):
            q2, x2 = (q + d) % 4, (x + d) % 4
            push(t_ref.at[pl.ds(q2 * 8 + s * 2, 2)], re1.at[q, two], 0, in_e1.at[s], (w, x, q2))
            push(t_ref.at[pl.ds(32 + x2 * 8 + s * 2, 2)], rq1.at[two, x], 1, in_q1.at[s], (w, x2, q))
        pltpu.make_async_copy(t_ref.at[pl.ds(q * 8 + s * 2, 2)], re1.at[q, two], in_e1.at[s]).start()
        pltpu.make_async_copy(t_ref.at[pl.ds(32 + x * 8 + s * 2, 2)], rq1.at[two, x], in_q1.at[s]).start()
        return _

    lax.fori_loop(0, STEPS, first, 0)

    def columns(target, value):
        high, low = halves(value)
        target[0:512, :] = high
        target[512:1024, :] = low
        target[1024:1536, :] = high

    def rows(target, value):
        high, low = halves(value)
        target[:, 0:512] = high
        target[:, 512:1024] = high
        target[:, 1024:1536] = low

    loads[0].wait()
    columns(b3c, b3f[...])
    loads[1].wait()
    rows(b2tl, b2f[...].T)

    def data_left(piece, factor):
        for k in range(4):
            high, low = halves(piece(k))
            lhs[:, k * 128 : k * 128 + 128] = high
            lhs[:, 512 + k * 128 : 640 + k * 128] = high
            lhs[:, 1024 + k * 128 : 1152 + k * 128] = low
        return jnp.dot(lhs[...], factor[...], preferred_element_type=F32)

    def data_right(factor, piece):
        for k in range(2):
            high, low = halves(piece(k))
            lanes = slice(k * 128, k * 128 + 128)
            rhs[0:512, lanes] = high
            rhs[512:1024, lanes] = low
            rhs[1024:1536, lanes] = high
        return jnp.dot(factor[...], rhs[...], preferred_element_type=F32)

    def stage_one(s, _):
        two = pl.ds(s * 2, 2)
        await_bytes(re1.at[:, two], in_e1.at[s])
        out = data_left(lambda k: re1[k, two].reshape(256, 128), b3c)
        for n in range(4):
            se2[n, two] = out[:, n * 128 : n * 128 + 128].reshape(2, 128, 128)
        for d in (2, 1, 3):
            x2 = (x + d) % 4
            push(se2.at[x2, two], re2.at[two, x], 2, in_e2.at[s], (w, x2, q))
        re2[two, x] = se2[x, two]

        await_bytes(rq1.at[two], in_q1.at[s])
        out = data_right(b2tl, lambda k: rq1[s * 2 + k].reshape(512, 128))
        sq2[s * 2] = out[:, 0:128]
        sq2[s * 2 + 1] = out[:, 128:256]

        def spread(n, _):
            w2, q2 = far(n)
            push(
                sq2.at[two, pl.ds((w2 * 4 + q2) * 16, 16)], rq2.at[q, w, two],
                3, in_q2.at[s], (w2, x, q2),
            )
            return _

        lax.fori_loop(1, 32, spread, 0)
        rq2[q, w, two] = sq2[two, pl.ds(pl.multiple_of(beta * 16, 16), 16)]
        return _

    lax.fori_loop(0, STEPS, stage_one, 0)

    loads[2].wait()
    rows(b1tl, b1f[...].T)
    rows(b1l, b1f[...])
    e1b[...] = jnp.broadcast_to(e1_ref[...], (128, DEPTH)).T

    def stage_two(s, _):
        two = pl.ds(s * 2, 2)
        await_bytes(re2.at[two, pl.ds(0, 3)], in_e2.at[s])
        out = data_right(b2tl, lambda k: re2[s * 2 + k].reshape(512, 128))
        se3[s * 2] = out[:, 0:128]
        se3[s * 2 + 1] = out[:, 128:256]

        def spread(n, _):
            w2, q2 = far(n)
            push(
                se3.at[two, pl.ds((w2 * 4 + q2) * 16, 16)], r3.at[w, 0, q, two],
                4, in_mid.at[0], (w2, x, q2),
            )
            return _

        lax.fori_loop(1, 32, spread, 0)
        r3[w, 0, q, two] = se3[two, pl.ds(pl.multiple_of(beta * 16, 16), 16)]

        await_bytes(sq2.at[pl.ds(0, 2), pl.ds(0, 496)], in_q2.at[s])
        out = data_left(lambda k: rq2[k, :, two].reshape(256, 128), b3c)
        for n in range(4):
            sq3[n, :, two] = out[:, n * 128 : n * 128 + 128].reshape(8, 2, 16, 128)
        for d in (2, 1, 3):
            x2 = (x + d) % 4
            push(sq3.at[x2, :, two], r3.at[:, 1, x, two], 5, in_mid.at[1], (w, x2, q))
        r3[:, 1, x, two] = sq3[x, :, two]
        return _

    lax.fori_loop(0, STEPS, stage_two, 0)

    rows(b2l, b2f[...])
    columns(b3tc, b3f[...].T)

    await_bytes(se3.at[:, pl.ds(0, 496)], in_mid.at[0])
    await_bytes(sq3.at[pl.ds(0, 3)], in_mid.at[1])

    flat = r3.reshape(8192, 128)
    along = e3_ref[pl.ds(x, 1), :]

    def middle(t, _):
        for pair in range(2):
            at = t * 4 + pair * 2
            rotated = data_right(b1tl, lambda k: flat[pl.ds(at + k, DEPTH, stride=16), :])
            scaled = []
            for k in range(2):
                spectrum = e1b[...] * e2_ref[beta * 16 + at + k] * along + noise_ref[0]
                scaled.append(rotated[:, k * 128 : k * 128 + 128] / spectrum)
            out = data_right(b1l, lambda k: scaled[k])
            for k in range(2):
                s3[at + k] = out[:, k * 128 : k * 128 + 128].reshape(8, 2, 4, 8, 128)
        four = pl.ds(t * 4, 4)
        for d in (2, 1, 3):
            x2 = (x + d) % 4
            push(s3.at[four, :, 1, x2], rq3p.at[x, four], 6, in_q3p.at[t], (w, x2, q))

        def spread(n, _):
            w2, q2 = far(n)
            push(s3.at[four, w2, 0, q2], re3p.at[beta, four], 7, in_e3p.at[0], (w2, x, q2))
            return _

        lax.fori_loop(1, 32, spread, 0)
        rq3p[x, four] = s3[four, :, 1, x]
        re3p[beta, four] = s3[four, w, 0, q]
        return _

    lax.fori_loop(0, STEPS, middle, 0)

    def back_q3(t, _):
        four = pl.ds(t * 4, 4)
        await_bytes(rq3p.at[pl.ds(0, 3), four], in_q3p.at[t])
        out = data_left(lambda k: rq3p[k, four].reshape(256, 128), b3tc)
        for n in range(4):
            sq2p[n, four] = out[:, n * 128 : n * 128 + 128].reshape(4, 8, 8, 128)

        def spread(n, _):
            w2, q2 = far(n)
            push(sq2p.at[q2, four, w2], rq2p.at[beta, four], 8, in_q2p.at[0], (w2, x, q2))
            return _

        lax.fori_loop(1, 32, spread, 0)
        rq2p[beta, four] = sq2p[q, four, w]
        return _

    lax.fori_loop(0, STEPS, back_q3, 0)

    await_bytes(re3p.at[pl.ds(0, 31)], in_e3p.at[0])
    flat_e = re3p.reshape(4096, 128)

    def back_e3(s, _):
        two = pl.ds(s * 2, 2)
        out = data_right(b2l, lambda k: flat_e[pl.ds(s * 2 + k, DEPTH, stride=8), :])
        for k in range(2):
            se2p[s * 2 + k] = out[:, k * 128 : k * 128 + 128].reshape(4, 128, 128)
        for d in (2, 1, 3):
            x2 = (x + d) % 4
            push(se2p.at[two, x2], re2p.at[x, two], 9, in_e2p.at[s], (w, x2, q))
        re2p[x, two] = se2p[two, x]
        return _

    lax.fori_loop(0, STEPS, back_e3, 0)

    def back_e2(s, _):
        two = pl.ds(s * 2, 2)
        await_bytes(re2p.at[pl.ds(0, 3), two], in_e2p.at[s])
        out = data_left(lambda k: re2p[k, two].reshape(256, 128), b3tc)
        for n in range(4):
            se1p[n, two] = out[:, n * 128 : n * 128 + 128].reshape(2, 128, 128)
        here = o_ref.at[pl.ds(q * 8 + s * 2, 2)]
        for d in (2, 1, 3):
            q2 = (q + d) % 4
            push(se1p.at[q2, two], here, 10, in_out.at[0], (w, x, q2))
        pltpu.make_async_copy(se1p.at[q, two], here, in_out.at[0]).start()
        return _

    lax.fori_loop(0, STEPS, back_e2, 0)

    await_bytes(rq2p.at[pl.ds(0, 31)], in_q2p.at[0])
    flat_q = rq2p.reshape(4096, 128)

    def back_q2(s, _):
        two = pl.ds(s * 2, 2)
        out = data_right(b2l, lambda k: flat_q[pl.ds(s * 2 + k, DEPTH, stride=8), :])
        for k in range(2):
            sq1p[s * 2 + k] = out[:, k * 128 : k * 128 + 128].reshape(4, 128, 128)
        here = o_ref.at[pl.ds(32 + x * 8 + s * 2, 2)]
        for d in (2, 1, 3):
            x2 = (x + d) % 4
            push(sq1p.at[two, x2], here, 11, in_out.at[1], (w, x2, q))
        pltpu.make_async_copy(sq1p.at[two, x], here, in_out.at[1]).start()
        return _

    lax.fori_loop(0, STEPS, back_q2, 0)

    await_bytes(re1, in_out.at[0])
    await_bytes(re1, in_out.at[1])
    for sem in (0, 1, 2, 5, 6, 9, 10, 11):
        await_bytes(re1.at[pl.ds(0, 3)], send.at[sem])
    for sem in (3, 4, 7, 8):
        await_bytes(rq2p.at[pl.ds(0, 31)], send.at[sem])


def per_device(targets, basis_first, basis_second, basis_third, eigen_first, eigen_second, eigen_third, noise):
    half = [
        (4, 8, 128, 128), (4, 8, 128, 128), (8, 4, 128, 128), (8, 512, 128),
        (8, 4, 128, 128), (8, 512, 128), (4, 8, 8, 16, 128), (4, 8, 8, 16, 128),
        (8, 2, 4, 8, 16, 128), (16, 8, 2, 4, 8, 128),
        (32, 16, 8, 128), (8, 4, 128, 128), (4, 8, 128, 128), (4, 8, 128, 128),
        (4, 16, 8, 8, 128), (4, 16, 8, 8, 128), (32, 16, 8, 128), (8, 4, 128, 128),
    ]
    scratch = [pltpu.VMEM(shape, F32) for shape in half]
    scratch += [pltpu.VMEM((512, 512), F32)] * 3
    scratch += [pltpu.VMEM((1536, 512), BF)] * 2 + [pltpu.VMEM((512, 1536), BF)] * 4
    scratch += [pltpu.VMEM((256, 1536), BF), pltpu.VMEM((1536, 256), BF), pltpu.VMEM((512, 128), F32)]
    dma = pltpu.SemaphoreType.DMA
    scratch += [dma((3,)), dma((12,))] + [dma((STEPS,))] * 4
    scratch += [dma((2,)), dma((1,)), dma((STEPS,)), dma((STEPS,)), dma((1,)), dma((2,))]
    whole = pl.BlockSpec(memory_space=pl.ANY)
    vmem = pl.BlockSpec(memory_space=pltpu.VMEM)
    smem = pl.BlockSpec(memory_space=pltpu.SMEM)
    return pl.pallas_call(
        kernel,
        out_shape=jax.ShapeDtypeStruct((64, 128, 128), F32),
        in_specs=[whole, whole, whole, whole, vmem, smem, vmem, smem],
        out_specs=whole,
        scratch_shapes=scratch,
        compiler_params=pltpu.CompilerParams(
            collective_id=0, has_side_effects=True, vmem_limit_bytes=67043328
        ),
        name="kron_solve",
    )(
        targets, basis_first, basis_second, basis_third,
        eigen_first.reshape(1, 512), eigen_second, eigen_third.reshape(4, 128), noise,
    )


def solution(mesh):
    in_specs = (P("gx", "gy", "gz"), P(), P(), P(), P(), P(), P(), P())
    return jax.shard_map(
        per_device, mesh=mesh, in_specs=in_specs, out_specs=P("gx", "gy", "gz"), check_vma=False
    )
```

```python
import functools

import jax
import jax.numpy as jnp
from jax import lax
from jax.experimental import pallas as pl
from jax.experimental.pallas import tpu as pltpu
from jax.sharding import PartitionSpec as P

MESH = pl.DeviceIdType.MESH
BF = jnp.bfloat16
F32 = jnp.float32
STEPS = 4
DEPTH = 512


def halves(value):
    high = value.astype(BF)
    return high, (value - high.astype(F32)).astype(BF)


def kernel(
    t_ref, b1_ref, b2_ref, b3_ref, e1_ref, e2_ref, e3_ref, noise_ref, o_ref,
    re1, se2, re2, se3, rq1, sq2, rq2, sq3, r3, s3,
    re3p, se2p, re2p, se1p, rq3p, sq2p, rq2p, sq1p,
    b1f, b2f, b3f, b3c, b3tc, b2l, b2tl, b1l, b1tl, lhs, rhs, mid, e1b,
    base_sem, send, in_e1, in_q1, in_e2, in_q2, in_mid, in_e3p, in_q3p, in_e2p, in_q2p, in_out,
):
    w, x, q = lax.axis_index("gx"), lax.axis_index("gy"), lax.axis_index("gz")
    y, z, core = w // 2, (q // 2) * 2 + w % 2, q % 2
    beta = w * 4 + q

    def far(n):
        pair = n // 2
        y2 = (y + pair % 4) % 4
        z2 = (z + pair % 4 + pair // 4) % 4
        c2 = (core + n % 2) % 2
        return y2 * 2 + z2 % 2, (z2 // 2) * 2 + c2

    def push(src, dst, sem, arrival, where):
        pltpu.make_async_remote_copy(
            src_ref=src, dst_ref=dst, send_sem=send.at[sem], recv_sem=arrival,
            device_id=where, device_id_type=MESH,
        ).start()

    def await_bytes(ref, sem):
        pltpu.make_async_copy(ref, ref, sem).wait()

    loads = [
        pltpu.make_async_copy(ref, buf, base_sem.at[n])
        for n, (ref, buf) in enumerate(((b3_ref, b3f), (b2_ref, b2f), (b1_ref, b1f)))
    ]
    for load in loads:
        load.start()

    barrier = pltpu.get_barrier_semaphore()

    def greet(n, _):
        w2, q2 = far(n)
        pl.semaphore_signal(barrier, inc=1, device_id=(w2, x, q2), device_id_type=MESH)
        return _

    for d in (1, 2, 3):
        pl.semaphore_signal(barrier, inc=1, device_id=(w, (x + d) % 4, q), device_id_type=MESH)
    lax.fori_loop(1, 32, greet, 0)
    pl.semaphore_wait(barrier, 34)

    def first(s, _):
        two = pl.ds(s * 2, 2)
        for d in (2, 1, 3):
            q2, x2 = (q + d) % 4, (x + d) % 4
            push(t_ref.at[pl.ds(q2 * 8 + s * 2, 2)], re1.at[q, two], 0, in_e1.at[s], (w, x, q2))
            push(t_ref.at[pl.ds(32 + x2 * 8 + s * 2, 2)], rq1.at[two, x], 1, in_q1.at[s], (w, x2, q))
        pltpu.make_async_copy(t_ref.at[pl.ds(q * 8 + s * 2, 2)], re1.at[q, two], in_e1.at[s]).start()
        pltpu.make_async_copy(t_ref.at[pl.ds(32 + x * 8 + s * 2, 2)], rq1.at[two, x], in_q1.at[s]).start()
        return _

    lax.fori_loop(0, STEPS, first, 0)

    def columns(target, value):
        high, low = halves(value)
        target[0:512, :] = high
        target[512:1024, :] = low
        target[1024:1536, :] = high

    def rows(target, value):
        high, low = halves(value)
        target[:, 0:512] = high
        target[:, 512:1024] = high
        target[:, 1024:1536] = low

    loads[0].wait()
    columns(b3c, b3f[...])
    loads[1].wait()
    rows(b2tl, b2f[...].T)

    def data_left(piece, factor):
        for k in range(4):
            high, low = halves(piece(k))
            lhs[:, k * 128 : k * 128 + 128] = high
            lhs[:, 512 + k * 128 : 640 + k * 128] = high
            lhs[:, 1024 + k * 128 : 1152 + k * 128] = low
        return jnp.dot(lhs[...], factor[...], preferred_element_type=F32)

    def data_right(factor, piece):
        for k in range(2):
            high, low = halves(piece(k))
            lanes = slice(k * 128, k * 128 + 128)
            rhs[0:512, lanes] = high
            rhs[512:1024, lanes] = low
            rhs[1024:1536, lanes] = high
        return jnp.dot(factor[...], rhs[...], preferred_element_type=F32)

    def stage_one(s, _):
        two = pl.ds(s * 2, 2)
        await_bytes(re1.at[:, two], in_e1.at[s])
        out = data_left(lambda k: re1[k, two].reshape(256, 128), b3c)
        for n in range(4):
            se2[n, two] = out[:, n * 128 : n * 128 + 128].reshape(2, 128, 128)
        for d in (2, 1, 3):
            x2 = (x + d) % 4
            push(se2.at[x2, two], re2.at[two, x], 2, in_e2.at[s], (w, x2, q))
        re2[two, x] = se2[x, two]

        await_bytes(rq1.at[two], in_q1.at[s])
        out = data_right(b2tl, lambda k: rq1[s * 2 + k].reshape(512, 128))
        sq2[s * 2] = out[:, 0:128]
        sq2[s * 2 + 1] = out[:, 128:256]

        def spread(n, _):
            w2, q2 = far(n)
            push(
                sq2.at[two, pl.ds((w2 * 4 + q2) * 16, 16)], rq2.at[q, w, two],
                3, in_q2.at[s], (w2, x, q2),
            )
            return _

        lax.fori_loop(1, 32, spread, 0)
        rq2[q, w, two] = sq2[two, pl.ds(pl.multiple_of(beta * 16, 16), 16)]
        return _

    lax.fori_loop(0, STEPS, stage_one, 0)

    loads[2].wait()
    rows(b1tl, b1f[...].T)
    place = lax.broadcasted_iota(jnp.int32, (DEPTH, DEPTH), 0)
    source = (place % 128) // 2 * 8 + place // 128 * 2 + place % 2
    pick = (lax.broadcasted_iota(jnp.int32, (DEPTH, DEPTH), 1) == source).astype(F32).astype(BF)
    high, low = halves(b1f[...])
    high = jnp.dot(pick, high, preferred_element_type=F32).astype(BF)
    low = jnp.dot(pick, low, preferred_element_type=F32).astype(BF)
    b1l[:, 0:512] = high
    b1l[:, 512:1024] = high
    b1l[:, 1024:1536] = low
    e1b[...] = jnp.broadcast_to(e1_ref[...], (128, DEPTH)).T

    def stage_two(s, _):
        two = pl.ds(s * 2, 2)
        await_bytes(re2.at[two, pl.ds(0, 3)], in_e2.at[s])
        out = data_right(b2tl, lambda k: re2[s * 2 + k].reshape(512, 128))
        se3[s * 2] = out[:, 0:128]
        se3[s * 2 + 1] = out[:, 128:256]

        def spread(n, _):
            w2, q2 = far(n)
            push(
                se3.at[two, pl.ds((w2 * 4 + q2) * 16, 16)], r3.at[w, 0, q, two],
                4, in_mid.at[0], (w2, x, q2),
            )
            return _

        lax.fori_loop(1, 32, spread, 0)
        r3[w, 0, q, two] = se3[two, pl.ds(pl.multiple_of(beta * 16, 16), 16)]

        await_bytes(sq2.at[pl.ds(0, 2), pl.ds(0, 496)], in_q2.at[s])
        out = data_left(lambda k: rq2[k, :, two].reshape(256, 128), b3c)
        for n in range(4):
            sq3[n, :, two] = out[:, n * 128 : n * 128 + 128].reshape(8, 2, 16, 128)
        for d in (2, 1, 3):
            x2 = (x + d) % 4
            push(sq3.at[x2, :, two], r3.at[:, 1, x, two], 5, in_mid.at[1], (w, x2, q))
        r3[:, 1, x, two] = sq3[x, :, two]
        return _

    lax.fori_loop(0, STEPS, stage_two, 0)

    rows(b2l, b2f[...])
    columns(b3tc, b3f[...].T)

    await_bytes(se3.at[:, pl.ds(0, 496)], in_mid.at[0])
    await_bytes(sq3.at[pl.ds(0, 3)], in_mid.at[1])

    flat = r3.reshape(8192, 128)
    flat_s = s3.reshape(8192, 128)
    along = e3_ref[pl.ds(x, 1), :]

    def middle(pair, _):
        at = pair * 2
        rotated = data_right(b1tl, lambda k: flat[pl.ds(at + k, DEPTH, stride=16), :])
        for k in range(2):
            lanes = slice(k * 128, k * 128 + 128)
            spectrum = e1b[...] * e2_ref[beta * 16 + at + k] * along + noise_ref[0]
            high, low = halves(rotated[:, lanes] / spectrum)
            mid[pair, 0:512, lanes] = high
            mid[pair, 512:1024, lanes] = low
            mid[pair, 1024:1536, lanes] = high
        return _

    lax.fori_loop(0, 8, middle, 0)

    def back_mid(s, _):
        factor = b1l[pl.ds(pl.multiple_of(s * 128, 128), 128), :]
        for pair in range(8):
            out = jnp.dot(factor, mid[pair], preferred_element_type=F32)
            for k in range(2):
                flat_s[pl.ds(s * 2048 + pair * 2 + k, 128, stride=16), :] = out[:, k * 128 : k * 128 + 128]
        for d in (2, 1, 3):
            x2 = (x + d) % 4
            push(s3.at[s, :, 1, x2], rq3p.at[x, s], 6, in_q3p.at[s], (w, x2, q))

        def spread(n, _):
            w2, q2 = far(n)
            push(
                s3.at[s, w2, 0, q2],
                re3p.at[pl.ds(s * 2, 2), pl.ds(pl.multiple_of(beta * 16, 16), 16)],
                7, in_e3p.at[s], (w2, x, q2),
            )
            return _

        lax.fori_loop(1, 32, spread, 0)
        rq3p[x, s] = s3[s, :, 1, x]
        re3p[pl.ds(s * 2, 2), pl.ds(pl.multiple_of(beta * 16, 16), 16)] = s3[s, w, 0, q]
        return _

    lax.fori_loop(0, STEPS, back_mid, 0)

    def back_one(s, _):
        two = pl.ds(s * 2, 2)
        await_bytes(se3.at[pl.ds(0, 2), pl.ds(0, 496)], in_e3p.at[s])
        out = data_right(b2l, lambda k: re3p[s * 2 + k])
        for k in range(2):
            se2p[s * 2 + k] = out[:, k * 128 : k * 128 + 128].reshape(4, 128, 128)
        for d in (2, 1, 3):
            x2 = (x + d) % 4
            push(se2p.at[two, x2], re2p.at[x, two], 9, in_e2p.at[s], (w, x2, q))
        re2p[x, two] = se2p[two, x]

        await_bytes(rq3p.at[pl.ds(0, 3), s], in_q3p.at[s])
        out = data_left(lambda k: rq3p[k, s].reshape(256, 128), b3tc)
        for n in range(4):
            sq2p[n, s] = out[:, n * 128 : n * 128 + 128].reshape(8, 2, 16, 128)

        def spread(n, _):
            w2, q2 = far(n)
            push(
                sq2p.at[q2, s, w2],
                rq2p.at[two, pl.ds(pl.multiple_of(beta * 16, 16), 16)],
                8, in_q2p.at[s], (w2, x, q2),
            )
            return _

        lax.fori_loop(1, 32, spread, 0)
        rq2p[two, pl.ds(pl.multiple_of(beta * 16, 16), 16)] = sq2p[q, s, w]
        return _

    lax.fori_loop(0, STEPS, back_one, 0)

    def back_two(s, _):
        two = pl.ds(s * 2, 2)
        await_bytes(re2p.at[pl.ds(0, 3), two], in_e2p.at[s])
        out = data_left(lambda k: re2p[k, two].reshape(256, 128), b3tc)
        for n in range(4):
            se1p[n, two] = out[:, n * 128 : n * 128 + 128].reshape(2, 128, 128)
        here = o_ref.at[pl.ds(q * 8 + s * 2, 2)]
        for d in (2, 1, 3):
            q2 = (q + d) % 4
            push(se1p.at[q2, two], here, 10, in_out.at[0], (w, x, q2))
        pltpu.make_async_copy(se1p.at[q, two], here, in_out.at[0]).start()

        await_bytes(se3.at[pl.ds(0, 2), pl.ds(0, 496)], in_q2p.at[s])
        out = data_right(b2l, lambda k: rq2p[s * 2 + k])
        for k in range(2):
            sq1p[s * 2 + k] = out[:, k * 128 : k * 128 + 128].reshape(4, 128, 128)
        here = o_ref.at[pl.ds(32 + x * 8 + s * 2, 2)]
        for d in (2, 1, 3):
            x2 = (x + d) % 4
            push(sq1p.at[two, x2], here, 11, in_out.at[1], (w, x2, q))
        pltpu.make_async_copy(sq1p.at[two, x], here, in_out.at[1]).start()
        return _

    lax.fori_loop(0, STEPS, back_two, 0)

    await_bytes(re1, in_out.at[0])
    await_bytes(re1, in_out.at[1])
    for sem in (0, 1, 2, 5, 6, 9, 10, 11):
        await_bytes(re1.at[pl.ds(0, 3)], send.at[sem])
    for sem in (3, 4, 7, 8):
        await_bytes(se3.at[:, pl.ds(0, 496)], send.at[sem])


def per_device(targets, basis_first, basis_second, basis_third, eigen_first, eigen_second, eigen_third, noise):
    half = [
        (4, 8, 128, 128), (4, 8, 128, 128), (8, 4, 128, 128), (8, 512, 128),
        (8, 4, 128, 128), (8, 512, 128), (4, 8, 8, 16, 128), (4, 8, 8, 16, 128),
        (8, 2, 4, 8, 16, 128), (4, 8, 2, 4, 2, 16, 128),
        (8, 512, 128), (8, 4, 128, 128), (4, 8, 128, 128), (4, 8, 128, 128),
        (4, 4, 8, 2, 16, 128), (4, 4, 8, 2, 16, 128), (8, 512, 128), (8, 4, 128, 128),
    ]
    scratch = [pltpu.VMEM(shape, F32) for shape in half]
    scratch += [pltpu.VMEM((512, 512), F32)] * 3
    scratch += [pltpu.VMEM((1536, 512), BF)] * 2 + [pltpu.VMEM((512, 1536), BF)] * 4
    scratch += [pltpu.VMEM((256, 1536), BF), pltpu.VMEM((1536, 256), BF)]
    scratch += [pltpu.VMEM((8, 1536, 256), BF), pltpu.VMEM((512, 128), F32)]
    dma = pltpu.SemaphoreType.DMA
    scratch += [dma((3,)), dma((12,))] + [dma((STEPS,))] * 4
    scratch += [dma((2,))] + [dma((STEPS,))] * 4 + [dma((2,))]
    whole = pl.BlockSpec(memory_space=pl.ANY)
    vmem = pl.BlockSpec(memory_space=pltpu.VMEM)
    smem = pl.BlockSpec(memory_space=pltpu.SMEM)
    return pl.pallas_call(
        kernel,
        out_shape=jax.ShapeDtypeStruct((64, 128, 128), F32),
        in_specs=[whole, whole, whole, whole, vmem, smem, vmem, smem],
        out_specs=whole,
        scratch_shapes=scratch,
        compiler_params=pltpu.CompilerParams(
            collective_id=0, has_side_effects=True, vmem_limit_bytes=67043328
        ),
        name="kron_solve",
    )(
        targets, basis_first, basis_second, basis_third,
        eigen_first.reshape(1, 512), eigen_second, eigen_third.reshape(4, 128), noise,
    )


def solution(mesh):
    in_specs = (P("gx", "gy", "gz"), P(), P(), P(), P(), P(), P(), P())
    return jax.shard_map(
        per_device, mesh=mesh, in_specs=in_specs, out_specs=P("gx", "gy", "gz"), check_vma=False
    )
```

```python
import functools

import jax
import jax.numpy as jnp
from jax import lax
from jax.experimental import pallas as pl
from jax.experimental.pallas import tpu as pltpu
from jax.sharding import PartitionSpec as P

MESH = pl.DeviceIdType.MESH
BF = jnp.bfloat16
F32 = jnp.float32
STEPS = 4
DEPTH = 512
ORDER = ("qe", "eq", "eq", "eq")


def halves(value):
    high = value.astype(BF)
    return high, (value - high.astype(F32)).astype(BF)


def kernel(
    t_ref, b1_ref, b2_ref, b3_ref, e1_ref, e2_ref, e3_ref, noise_ref, o_ref,
    re1, se2, re2, se3, rq1, sq2, rq2, sq3, r3, s3,
    re3p, se2p, re2p, se1p, rq3p, sq2p, rq2p, sq1p,
    b1f, b2f, b3f, b3c, b3tc, b2l, b2tl, b1l, b1tl, lhs, rhs, mid, e1b,
    base_sem, send, in_e1, in_q1, in_e2, in_q2, in_mid, in_e3p, in_q3p, in_e2p, in_q2p, in_out,
):
    w, x, q = lax.axis_index("gx"), lax.axis_index("gy"), lax.axis_index("gz")
    y, z, core = w // 2, (q // 2) * 2 + w % 2, q % 2
    beta = w * 4 + q

    def far(dy, dz, dc):
        y2, z2, c2 = (y + dy) % 4, (z + dz) % 4, (core + dc) % 2
        return y2 * 2 + z2 % 2, (z2 // 2) * 2 + c2

    def each_far(act):
        def both(n, _):
            k = n // 2
            act(*far(k % 3 + 1, (k % 3 + k // 3) % 3 + 1, n % 2))
            return _

        def one(n, _):
            act(*far(n // 2 + 1, 0, n % 2))
            return _

        def other(n, _):
            act(*far(0, n // 2 + 1, n % 2))
            return _

        lax.fori_loop(0, 18, both, 0)
        lax.fori_loop(0, 6, one, 0)
        lax.fori_loop(0, 6, other, 0)
        act(*far(0, 0, 1))

    def push(src, dst, sem, arrival, where):
        pltpu.make_async_remote_copy(
            src_ref=src, dst_ref=dst, send_sem=send.at[sem], recv_sem=arrival,
            device_id=where, device_id_type=MESH,
        ).start()

    def await_bytes(ref, sem):
        pltpu.make_async_copy(ref, ref, sem).wait()

    def staged(part_e, part_q, order):
        def body(s, _):
            for part in order:
                (part_e if part == "e" else part_q)(s)
            return _

        lax.fori_loop(0, STEPS, body, 0)

    loads = [
        pltpu.make_async_copy(ref, buf, base_sem.at[n])
        for n, (ref, buf) in enumerate(((b3_ref, b3f), (b2_ref, b2f), (b1_ref, b1f)))
    ]
    for load in loads:
        load.start()

    barrier = pltpu.get_barrier_semaphore()

    def greet(w2, q2):
        pl.semaphore_signal(barrier, inc=1, device_id=(w2, x, q2), device_id_type=MESH)

    for d in (1, 2, 3):
        pl.semaphore_signal(barrier, inc=1, device_id=(w, (x + d) % 4, q), device_id_type=MESH)
    each_far(greet)
    pl.semaphore_wait(barrier, 34)

    def first(s, _):
        two = pl.ds(s * 2, 2)
        for d in (2, 1, 3):
            q2, x2 = (q + d) % 4, (x + d) % 4
            push(t_ref.at[pl.ds(q2 * 8 + s * 2, 2)], re1.at[q, two], 0, in_e1.at[s], (w, x, q2))
            push(t_ref.at[pl.ds(32 + x2 * 8 + s * 2, 2)], rq1.at[two, x], 1, in_q1.at[s], (w, x2, q))
        pltpu.make_async_copy(t_ref.at[pl.ds(q * 8 + s * 2, 2)], re1.at[q, two], in_e1.at[s]).start()
        pltpu.make_async_copy(t_ref.at[pl.ds(32 + x * 8 + s * 2, 2)], rq1.at[two, x], in_q1.at[s]).start()
        return _

    lax.fori_loop(0, STEPS, first, 0)

    def columns(target, value):
        high, low = halves(value)
        target[0:512, :] = high
        target[512:1024, :] = low
        target[1024:1536, :] = high

    def rows(target, value):
        high, low = halves(value)
        target[:, 0:512] = high
        target[:, 512:1024] = high
        target[:, 1024:1536] = low

    loads[0].wait()
    columns(b3c, b3f[...])
    loads[1].wait()
    rows(b2tl, b2f[...].T)

    def data_left(piece, factor):
        for k in range(4):
            high, low = halves(piece(k))
            lhs[:, k * 128 : k * 128 + 128] = high
            lhs[:, 512 + k * 128 : 640 + k * 128] = high
            lhs[:, 1024 + k * 128 : 1152 + k * 128] = low
        return jnp.dot(lhs[...], factor[...], preferred_element_type=F32)

    def data_right(factor, piece):
        for k in range(2):
            high, low = halves(piece(k))
            lanes = slice(k * 128, k * 128 + 128)
            rhs[0:512, lanes] = high
            rhs[512:1024, lanes] = low
            rhs[1024:1536, lanes] = high
        return jnp.dot(factor[...], rhs[...], preferred_element_type=F32)

    def stage_one_e(s):
        two = pl.ds(s * 2, 2)
        await_bytes(re1.at[:, two], in_e1.at[s])
        out = data_left(lambda k: re1[k, two].reshape(256, 128), b3c)
        for n in range(4):
            se2[n, two] = out[:, n * 128 : n * 128 + 128].reshape(2, 128, 128)
        for d in (2, 1, 3):
            x2 = (x + d) % 4
            push(se2.at[x2, two], re2.at[two, x], 2, in_e2.at[s], (w, x2, q))
        re2[two, x] = se2[x, two]

    def stage_one_q(s):
        two = pl.ds(s * 2, 2)
        await_bytes(rq1.at[two], in_q1.at[s])
        out = data_right(b2tl, lambda k: rq1[s * 2 + k].reshape(512, 128))
        sq2[s * 2] = out[:, 0:128]
        sq2[s * 2 + 1] = out[:, 128:256]

        def spread(w2, q2):
            push(
                sq2.at[two, pl.ds((w2 * 4 + q2) * 16, 16)], rq2.at[q, w, two],
                3, in_q2.at[s], (w2, x, q2),
            )

        each_far(spread)
        rq2[q, w, two] = sq2[two, pl.ds(pl.multiple_of(beta * 16, 16), 16)]

    staged(stage_one_e, stage_one_q, ORDER[0])

    loads[2].wait()
    rows(b1tl, b1f[...].T)
    place = lax.broadcasted_iota(jnp.int32, (DEPTH, DEPTH), 0)
    source = (place % 128) // 2 * 8 + place // 128 * 2 + place % 2
    pick = (lax.broadcasted_iota(jnp.int32, (DEPTH, DEPTH), 1) == source).astype(F32).astype(BF)
    high, low = halves(b1f[...])
    high = jnp.dot(pick, high, preferred_element_type=F32).astype(BF)
    low = jnp.dot(pick, low, preferred_element_type=F32).astype(BF)
    b1l[:, 0:512] = high
    b1l[:, 512:1024] = high
    b1l[:, 1024:1536] = low
    e1b[...] = jnp.broadcast_to(e1_ref[...], (128, DEPTH)).T

    def stage_two_e(s):
        two = pl.ds(s * 2, 2)
        await_bytes(re2.at[two, pl.ds(0, 3)], in_e2.at[s])
        out = data_right(b2tl, lambda k: re2[s * 2 + k].reshape(512, 128))
        se3[s * 2] = out[:, 0:128]
        se3[s * 2 + 1] = out[:, 128:256]

        def spread(w2, q2):
            push(
                se3.at[two, pl.ds((w2 * 4 + q2) * 16, 16)], r3.at[w, 0, q, two],
                4, in_mid.at[0], (w2, x, q2),
            )

        each_far(spread)
        r3[w, 0, q, two] = se3[two, pl.ds(pl.multiple_of(beta * 16, 16), 16)]

    def stage_two_q(s):
        two = pl.ds(s * 2, 2)
        await_bytes(sq2.at[pl.ds(0, 2), pl.ds(0, 496)], in_q2.at[s])
        out = data_left(lambda k: rq2[k, :, two].reshape(256, 128), b3c)
        for n in range(4):
            sq3[n, :, two] = out[:, n * 128 : n * 128 + 128].reshape(8, 2, 16, 128)
        for d in (2, 1, 3):
            x2 = (x + d) % 4
            push(sq3.at[x2, :, two], r3.at[:, 1, x, two], 5, in_mid.at[1], (w, x2, q))
        r3[:, 1, x, two] = sq3[x, :, two]

    staged(stage_two_e, stage_two_q, ORDER[1])

    rows(b2l, b2f[...])
    columns(b3tc, b3f[...].T)

    await_bytes(se3.at[:, pl.ds(0, 496)], in_mid.at[0])
    await_bytes(sq3.at[pl.ds(0, 3)], in_mid.at[1])

    flat = r3.reshape(8192, 128)
    flat_s = s3.reshape(8192, 128)
    along = e3_ref[pl.ds(x, 1), :]

    def middle(pair, _):
        at = pair * 2
        rotated = data_right(b1tl, lambda k: flat[pl.ds(at + k, DEPTH, stride=16), :])
        for k in range(2):
            lanes = slice(k * 128, k * 128 + 128)
            spectrum = e1b[...] * e2_ref[beta * 16 + at + k] * along + noise_ref[0]
            high, low = halves(rotated[:, lanes] / spectrum)
            mid[pair, 0:512, lanes] = high
            mid[pair, 512:1024, lanes] = low
            mid[pair, 1024:1536, lanes] = high
        return _

    lax.fori_loop(0, 8, middle, 0)

    def back_mid(s, _):
        factor = b1l[pl.ds(pl.multiple_of(s * 128, 128), 128), :]
        for pair in range(8):
            out = jnp.dot(factor, mid[pair], preferred_element_type=F32)
            for k in range(2):
                flat_s[pl.ds(s * 2048 + pair * 2 + k, 128, stride=16), :] = out[:, k * 128 : k * 128 + 128]
        for d in (2, 1, 3):
            x2 = (x + d) % 4
            push(s3.at[s, :, 1, x2], rq3p.at[x, s], 6, in_q3p.at[s], (w, x2, q))

        def spread(w2, q2):
            push(
                s3.at[s, w2, 0, q2],
                re3p.at[pl.ds(s * 2, 2), pl.ds(pl.multiple_of(beta * 16, 16), 16)],
                7, in_e3p.at[s], (w2, x, q2),
            )

        each_far(spread)
        rq3p[x, s] = s3[s, :, 1, x]
        re3p[pl.ds(s * 2, 2), pl.ds(pl.multiple_of(beta * 16, 16), 16)] = s3[s, w, 0, q]
        return _

    lax.fori_loop(0, STEPS, back_mid, 0)

    def back_one_e(s):
        two = pl.ds(s * 2, 2)
        await_bytes(se3.at[pl.ds(0, 2), pl.ds(0, 496)], in_e3p.at[s])
        out = data_right(b2l, lambda k: re3p[s * 2 + k])
        for k in range(2):
            se2p[s * 2 + k] = out[:, k * 128 : k * 128 + 128].reshape(4, 128, 128)
        for d in (2, 1, 3):
            x2 = (x + d) % 4
            push(se2p.at[two, x2], re2p.at[x, two], 9, in_e2p.at[s], (w, x2, q))
        re2p[x, two] = se2p[two, x]

    def back_one_q(s):
        two = pl.ds(s * 2, 2)
        await_bytes(rq3p.at[pl.ds(0, 3), s], in_q3p.at[s])
        out = data_left(lambda k: rq3p[k, s].reshape(256, 128), b3tc)
        for n in range(4):
            sq2p[n, s] = out[:, n * 128 : n * 128 + 128].reshape(8, 2, 16, 128)

        def spread(w2, q2):
            push(
                sq2p.at[q2, s, w2],
                rq2p.at[two, pl.ds(pl.multiple_of(beta * 16, 16), 16)],
                8, in_q2p.at[s], (w2, x, q2),
            )

        each_far(spread)
        rq2p[two, pl.ds(pl.multiple_of(beta * 16, 16), 16)] = sq2p[q, s, w]

    staged(back_one_e, back_one_q, ORDER[2])

    def back_two_e(s):
        two = pl.ds(s * 2, 2)
        await_bytes(re2p.at[pl.ds(0, 3), two], in_e2p.at[s])
        out = data_left(lambda k: re2p[k, two].reshape(256, 128), b3tc)
        for n in range(4):
            se1p[n, two] = out[:, n * 128 : n * 128 + 128].reshape(2, 128, 128)
        here = o_ref.at[pl.ds(q * 8 + s * 2, 2)]
        for d in (2, 1, 3):
            q2 = (q + d) % 4
            push(se1p.at[q2, two], here, 10, in_out.at[0], (w, x, q2))
        pltpu.make_async_copy(se1p.at[q, two], here, in_out.at[0]).start()

    def back_two_q(s):
        two = pl.ds(s * 2, 2)
        await_bytes(se3.at[pl.ds(0, 2), pl.ds(0, 496)], in_q2p.at[s])
        out = data_right(b2l, lambda k: rq2p[s * 2 + k])
        for k in range(2):
            sq1p[s * 2 + k] = out[:, k * 128 : k * 128 + 128].reshape(4, 128, 128)
        here = o_ref.at[pl.ds(32 + x * 8 + s * 2, 2)]
        for d in (2, 1, 3):
            x2 = (x + d) % 4
            push(sq1p.at[two, x2], here, 11, in_out.at[1], (w, x2, q))
        pltpu.make_async_copy(sq1p.at[two, x], here, in_out.at[1]).start()

    staged(back_two_e, back_two_q, ORDER[3])

    await_bytes(re1, in_out.at[0])
    await_bytes(re1, in_out.at[1])
    for sem in (0, 1, 2, 5, 6, 9, 10, 11):
        await_bytes(re1.at[pl.ds(0, 3)], send.at[sem])
    for sem in (3, 4, 7, 8):
        await_bytes(se3.at[:, pl.ds(0, 496)], send.at[sem])


def per_device(targets, basis_first, basis_second, basis_third, eigen_first, eigen_second, eigen_third, noise):
    half = [
        (4, 8, 128, 128), (4, 8, 128, 128), (8, 4, 128, 128), (8, 512, 128),
        (8, 4, 128, 128), (8, 512, 128), (4, 8, 8, 16, 128), (4, 8, 8, 16, 128),
        (8, 2, 4, 8, 16, 128), (4, 8, 2, 4, 2, 16, 128),
        (8, 512, 128), (8, 4, 128, 128), (4, 8, 128, 128), (4, 8, 128, 128),
        (4, 4, 8, 2, 16, 128), (4, 4, 8, 2, 16, 128), (8, 512, 128), (8, 4, 128, 128),
    ]
    scratch = [pltpu.VMEM(shape, F32) for shape in half]
    scratch += [pltpu.VMEM((512, 512), F32)] * 3
    scratch += [pltpu.VMEM((1536, 512), BF)] * 2 + [pltpu.VMEM((512, 1536), BF)] * 4
    scratch += [pltpu.VMEM((256, 1536), BF), pltpu.VMEM((1536, 256), BF)]
    scratch += [pltpu.VMEM((8, 1536, 256), BF), pltpu.VMEM((512, 128), F32)]
    dma = pltpu.SemaphoreType.DMA
    scratch += [dma((3,)), dma((12,))] + [dma((STEPS,))] * 4
    scratch += [dma((2,))] + [dma((STEPS,))] * 4 + [dma((2,))]
    whole = pl.BlockSpec(memory_space=pl.ANY)
    vmem = pl.BlockSpec(memory_space=pltpu.VMEM)
    smem = pl.BlockSpec(memory_space=pltpu.SMEM)
    return pl.pallas_call(
        kernel,
        out_shape=jax.ShapeDtypeStruct((64, 128, 128), F32),
        in_specs=[whole, whole, whole, whole, vmem, smem, vmem, smem],
        out_specs=whole,
        scratch_shapes=scratch,
        compiler_params=pltpu.CompilerParams(
            collective_id=0, has_side_effects=True, vmem_limit_bytes=67043328
        ),
        name="kron_solve",
    )(
        targets, basis_first, basis_second, basis_third,
        eigen_first.reshape(1, 512), eigen_second, eigen_third.reshape(4, 128), noise,
    )


def solution(mesh):
    in_specs = (P("gx", "gy", "gz"), P(), P(), P(), P(), P(), P(), P())
    return jax.shard_map(
        per_device, mesh=mesh, in_specs=in_specs, out_specs=P("gx", "gy", "gz"), check_vma=False
    )
```

```python
import functools

import jax
import jax.numpy as jnp
from jax import lax
from jax.experimental import pallas as pl
from jax.experimental.pallas import tpu as pltpu
from jax.sharding import PartitionSpec as P

MESH = pl.DeviceIdType.MESH
BF = jnp.bfloat16
F32 = jnp.float32
STEPS = 4
DEPTH = 512
ORDER = ("qe", "eq", "eq", "eq")


def halves(value):
    high = value.astype(BF)
    return high, (value - high.astype(F32)).astype(BF)


def kernel(
    t_ref, b1_ref, b2_ref, b3_ref, e1_ref, e2_ref, e3_ref, noise_ref, o_ref,
    re1, se2, re2, se3, rq1, sq2, rq2, sq3, r3, s3,
    re3p, se2p, re2p, se1p, rq3p, sq2p, rq2p, sq1p,
    b1f, b2f, b3f, b3c, b3tc, b2l, b2tl, b1l, b1tm, lhs, rhs, mid, e1b,
    base_sem, send, in_e1, in_q1, in_e2, in_q2, in_me, in_mq, in_e3p, in_q3p, in_e2p, in_q2p, in_out,
):
    w, x, q = lax.axis_index("gx"), lax.axis_index("gy"), lax.axis_index("gz")
    y, z, core = w // 2, (q // 2) * 2 + w % 2, q % 2
    beta = w * 4 + q

    def far(dy, dz, dc):
        y2, z2, c2 = (y + dy) % 4, (z + dz) % 4, (core + dc) % 2
        return y2 * 2 + z2 % 2, (z2 // 2) * 2 + c2

    def each_far(act):
        def both(n, _):
            k = n // 2
            act(*far(k % 3 + 1, (k % 3 + k // 3) % 3 + 1, n % 2))
            return _

        def one(n, _):
            act(*far(n // 2 + 1, 0, n % 2))
            return _

        def other(n, _):
            act(*far(0, n // 2 + 1, n % 2))
            return _

        lax.fori_loop(0, 18, both, 0)
        lax.fori_loop(0, 6, one, 0)
        lax.fori_loop(0, 6, other, 0)
        act(*far(0, 0, 1))

    def push(src, dst, sem, arrival, where):
        pltpu.make_async_remote_copy(
            src_ref=src, dst_ref=dst, send_sem=send.at[sem], recv_sem=arrival,
            device_id=where, device_id_type=MESH,
        ).start()

    def await_bytes(ref, sem):
        pltpu.make_async_copy(ref, ref, sem).wait()

    def staged(part_e, part_q, order):
        def body(s, _):
            for part in order:
                (part_e if part == "e" else part_q)(s)
            return _

        lax.fori_loop(0, STEPS, body, 0)

    loads = [
        pltpu.make_async_copy(ref, buf, base_sem.at[n])
        for n, (ref, buf) in enumerate(((b3_ref, b3f), (b2_ref, b2f), (b1_ref, b1f)))
    ]
    for load in loads:
        load.start()

    barrier = pltpu.get_barrier_semaphore()

    def greet(w2, q2):
        pl.semaphore_signal(barrier, inc=1, device_id=(w2, x, q2), device_id_type=MESH)

    for d in (1, 2, 3):
        pl.semaphore_signal(barrier, inc=1, device_id=(w, (x + d) % 4, q), device_id_type=MESH)
    each_far(greet)
    pl.semaphore_wait(barrier, 34)

    def first(s, _):
        two = pl.ds(s * 2, 2)
        for d in (2, 1, 3):
            q2, x2 = (q + d) % 4, (x + d) % 4
            push(t_ref.at[pl.ds(q2 * 8 + s * 2, 2)], re1.at[q, two], 0, in_e1.at[s], (w, x, q2))
            push(t_ref.at[pl.ds(32 + x2 * 8 + s * 2, 2)], rq1.at[two, x], 1, in_q1.at[s], (w, x2, q))
        pltpu.make_async_copy(t_ref.at[pl.ds(q * 8 + s * 2, 2)], re1.at[q, two], in_e1.at[s]).start()
        pltpu.make_async_copy(t_ref.at[pl.ds(32 + x * 8 + s * 2, 2)], rq1.at[two, x], in_q1.at[s]).start()
        return _

    lax.fori_loop(0, STEPS, first, 0)

    def columns(target, value):
        high, low = halves(value)
        target[0:512, :] = high
        target[512:1024, :] = low
        target[1024:1536, :] = high

    def rows(target, value):
        high, low = halves(value)
        target[:, 0:512] = high
        target[:, 512:1024] = high
        target[:, 1024:1536] = low

    loads[0].wait()
    columns(b3c, b3f[...])
    loads[1].wait()
    rows(b2tl, b2f[...].T)

    def data_left(piece, factor):
        for k in range(4):
            high, low = halves(piece(k))
            lhs[:, k * 128 : k * 128 + 128] = high
            lhs[:, 512 + k * 128 : 640 + k * 128] = high
            lhs[:, 1024 + k * 128 : 1152 + k * 128] = low
        return jnp.dot(lhs[...], factor[...], preferred_element_type=F32)

    def data_right(factor, piece):
        for k in range(2):
            high, low = halves(piece(k))
            lanes = slice(k * 128, k * 128 + 128)
            rhs[0:512, lanes] = high
            rhs[512:1024, lanes] = low
            rhs[1024:1536, lanes] = high
        return jnp.dot(factor[...], rhs[...], preferred_element_type=F32)

    def stage_one_e(s):
        two = pl.ds(s * 2, 2)
        await_bytes(re1.at[:, two], in_e1.at[s])
        out = data_left(lambda k: re1[k, two].reshape(256, 128), b3c)
        for n in range(4):
            se2[n, two] = out[:, n * 128 : n * 128 + 128].reshape(2, 128, 128)
        for d in (2, 1, 3):
            x2 = (x + d) % 4
            push(se2.at[x2, two], re2.at[two, x], 2, in_e2.at[s], (w, x2, q))
        re2[two, x] = se2[x, two]

    def stage_one_q(s):
        two = pl.ds(s * 2, 2)
        await_bytes(rq1.at[two], in_q1.at[s])
        out = data_right(b2tl, lambda k: rq1[s * 2 + k].reshape(512, 128))
        sq2[s * 2] = out[:, 0:128]
        sq2[s * 2 + 1] = out[:, 128:256]

        def spread(w2, q2):
            push(
                sq2.at[two, pl.ds((w2 * 4 + q2) * 16, 16)], rq2.at[q, w, two],
                3, in_q2.at[s], (w2, x, q2),
            )

        each_far(spread)
        rq2[q, w, two] = sq2[two, pl.ds(pl.multiple_of(beta * 16, 16), 16)]

    staged(stage_one_e, stage_one_q, ORDER[0])

    loads[2].wait()
    place = lax.broadcasted_iota(jnp.int32, (DEPTH, DEPTH), 0)
    source = (place % 128) // 2 * 8 + place // 128 * 2 + place % 2
    pick = (lax.broadcasted_iota(jnp.int32, (DEPTH, DEPTH), 1) == source).astype(F32).astype(BF)
    high, low = halves(b1f[...])
    high = jnp.dot(pick, high, preferred_element_type=F32)
    low = jnp.dot(pick, low, preferred_element_type=F32)
    b1l[:, 0:512] = high.astype(BF)
    b1l[:, 512:1024] = high.astype(BF)
    b1l[:, 1024:1536] = low.astype(BF)
    high, low = high.T.astype(BF), low.T.astype(BF)
    for n in range(STEPS):
        b1tm[n, :, 0:128] = high[:, n * 128 : n * 128 + 128]
        b1tm[n, :, 128:256] = high[:, n * 128 : n * 128 + 128]
        b1tm[n, :, 256:384] = low[:, n * 128 : n * 128 + 128]
    s3[...] = jnp.zeros_like(s3)
    e1b[...] = jnp.broadcast_to(e1_ref[...], (128, DEPTH)).T

    def stage_two_e(s):
        two = pl.ds(s * 2, 2)
        await_bytes(re2.at[two, pl.ds(0, 3)], in_e2.at[s])
        out = data_right(b2tl, lambda k: re2[s * 2 + k].reshape(512, 128))
        se3[s * 2] = out[:, 0:128]
        se3[s * 2 + 1] = out[:, 128:256]

        def spread(w2, q2):
            push(
                se3.at[two, pl.ds((w2 * 4 + q2) * 16, 16)], r3.at[s, w, 0, q],
                4, in_me.at[s], (w2, x, q2),
            )

        each_far(spread)
        r3[s, w, 0, q] = se3[two, pl.ds(pl.multiple_of(beta * 16, 16), 16)]

    def stage_two_q(s):
        two = pl.ds(s * 2, 2)
        await_bytes(sq2.at[pl.ds(0, 2), pl.ds(0, 496)], in_q2.at[s])
        out = data_left(lambda k: rq2[k, :, two].reshape(256, 128), b3c)
        for n in range(4):
            sq3[n, :, two] = out[:, n * 128 : n * 128 + 128].reshape(8, 2, 16, 128)
        for d in (2, 1, 3):
            x2 = (x + d) % 4
            push(sq3.at[x2, :, two], r3.at[s, :, 1, x], 5, in_mq.at[s], (w, x2, q))
        r3[s, :, 1, x] = sq3[x, :, two]

    staged(stage_two_e, stage_two_q, ORDER[1])

    rows(b2l, b2f[...])
    columns(b3tc, b3f[...].T)

    flat = r3.reshape(8192, 128)
    flat_s = s3.reshape(8192, 128)
    along = e3_ref[pl.ds(x, 1), :]

    def arrived(s):
        await_bytes(se3.at[pl.ds(0, 2), pl.ds(0, 496)], in_me.at[s])
        await_bytes(sq3.at[pl.ds(0, 3), :, pl.ds(0, 2)], in_mq.at[s])

    def term(s, pair):
        for k in range(2):
            high, low = halves(flat[pl.ds(s * 2048 + pair * 2 + k, 128, stride=16), :])
            lanes = slice(k * 128, k * 128 + 128)
            rhs[0:128, lanes] = high
            rhs[128:256, lanes] = low
            rhs[256:384, lanes] = high
        return jnp.dot(b1tm[s], rhs[0:384, :], preferred_element_type=F32)

    def total(at):
        return flat_s.at[pl.ds(pl.multiple_of(at * DEPTH, DEPTH), DEPTH), :]

    def gather_sum(s, _):
        arrived(s)

        def one_pair(pair, _):
            part = term(s, pair)
            for k in range(2):
                total(pair * 2 + k)[...] += part[:, k * 128 : k * 128 + 128]
            return _

        lax.fori_loop(0, 8, one_pair, 0)
        return _

    lax.fori_loop(0, STEPS - 1, gather_sum, 0)
    arrived(STEPS - 1)

    def middle(pair, _):
        part = term(STEPS - 1, pair)
        for k in range(2):
            at = pair * 2 + k
            lanes = slice(k * 128, k * 128 + 128)
            spectrum = e1b[...] * e2_ref[beta * 16 + at] * along + noise_ref[0]
            high, low = halves((total(at)[...] + part[:, lanes]) / spectrum)
            mid[pair, 0:512, lanes] = high
            mid[pair, 512:1024, lanes] = low
        return _

    lax.fori_loop(0, 8, middle, 0)

    def back_mid(s, _):
        factor = b1l[pl.ds(pl.multiple_of(s * 128, 128), 128), :]
        for pair in range(8):
            out = jnp.dot(factor[:, 0:1024], mid[pair], preferred_element_type=F32)
            out += jnp.dot(factor[:, 1024:1536], mid[pair, 0:512], preferred_element_type=F32)
            for k in range(2):
                flat_s[pl.ds(s * 2048 + pair * 2 + k, 128, stride=16), :] = out[:, k * 128 : k * 128 + 128]
        for d in (2, 1, 3):
            x2 = (x + d) % 4
            push(s3.at[s, :, 1, x2], rq3p.at[x, s], 6, in_q3p.at[s], (w, x2, q))

        def spread(w2, q2):
            push(
                s3.at[s, w2, 0, q2],
                re3p.at[pl.ds(s * 2, 2), pl.ds(pl.multiple_of(beta * 16, 16), 16)],
                7, in_e3p.at[s], (w2, x, q2),
            )

        each_far(spread)
        rq3p[x, s] = s3[s, :, 1, x]
        re3p[pl.ds(s * 2, 2), pl.ds(pl.multiple_of(beta * 16, 16), 16)] = s3[s, w, 0, q]
        return _

    lax.fori_loop(0, STEPS, back_mid, 0)

    def back_one_e(s):
        two = pl.ds(s * 2, 2)
        await_bytes(se3.at[pl.ds(0, 2), pl.ds(0, 496)], in_e3p.at[s])
        out = data_right(b2l, lambda k: re3p[s * 2 + k])
        for k in range(2):
            se2p[s * 2 + k] = out[:, k * 128 : k * 128 + 128].reshape(4, 128, 128)
        for d in (2, 1, 3):
            x2 = (x + d) % 4
            push(se2p.at[two, x2], re2p.at[x, two], 9, in_e2p.at[s], (w, x2, q))
        re2p[x, two] = se2p[two, x]

    def back_one_q(s):
        two = pl.ds(s * 2, 2)
        await_bytes(rq3p.at[pl.ds(0, 3), s], in_q3p.at[s])
        out = data_left(lambda k: rq3p[k, s].reshape(256, 128), b3tc)
        for n in range(4):
            sq2p[n, s] = out[:, n * 128 : n * 128 + 128].reshape(8, 2, 16, 128)

        def spread(w2, q2):
            push(
                sq2p.at[q2, s, w2],
                rq2p.at[two, pl.ds(pl.multiple_of(beta * 16, 16), 16)],
                8, in_q2p.at[s], (w2, x, q2),
            )

        each_far(spread)
        rq2p[two, pl.ds(pl.multiple_of(beta * 16, 16), 16)] = sq2p[q, s, w]

    staged(back_one_e, back_one_q, ORDER[2])

    def back_two_e(s):
        two = pl.ds(s * 2, 2)
        await_bytes(re2p.at[pl.ds(0, 3), two], in_e2p.at[s])
        out = data_left(lambda k: re2p[k, two].reshape(256, 128), b3tc)
        for n in range(4):
            se1p[n, two] = out[:, n * 128 : n * 128 + 128].reshape(2, 128, 128)
        here = o_ref.at[pl.ds(q * 8 + s * 2, 2)]
        for d in (2, 1, 3):
            q2 = (q + d) % 4
            push(se1p.at[q2, two], here, 10, in_out.at[0], (w, x, q2))
        pltpu.make_async_copy(se1p.at[q, two], here, in_out.at[0]).start()

    def back_two_q(s):
        two = pl.ds(s * 2, 2)
        await_bytes(se3.at[pl.ds(0, 2), pl.ds(0, 496)], in_q2p.at[s])
        out = data_right(b2l, lambda k: rq2p[s * 2 + k])
        for k in range(2):
            sq1p[s * 2 + k] = out[:, k * 128 : k * 128 + 128].reshape(4, 128, 128)
        here = o_ref.at[pl.ds(32 + x * 8 + s * 2, 2)]
        for d in (2, 1, 3):
            x2 = (x + d) % 4
            push(sq1p.at[two, x2], here, 11, in_out.at[1], (w, x2, q))
        pltpu.make_async_copy(sq1p.at[two, x], here, in_out.at[1]).start()

    staged(back_two_e, back_two_q, ORDER[3])

    await_bytes(re1, in_out.at[0])
    await_bytes(re1, in_out.at[1])
    for sem in (0, 1, 2, 5, 6, 9, 10, 11):
        await_bytes(re1.at[pl.ds(0, 3)], send.at[sem])
    for sem in (3, 4, 7, 8):
        await_bytes(se3.at[:, pl.ds(0, 496)], send.at[sem])


def per_device(targets, basis_first, basis_second, basis_third, eigen_first, eigen_second, eigen_third, noise):
    half = [
        (4, 8, 128, 128), (4, 8, 128, 128), (8, 4, 128, 128), (8, 512, 128),
        (8, 4, 128, 128), (8, 512, 128), (4, 8, 8, 16, 128), (4, 8, 8, 16, 128),
        (4, 8, 2, 4, 2, 16, 128), (4, 8, 2, 4, 2, 16, 128),
        (8, 512, 128), (8, 4, 128, 128), (4, 8, 128, 128), (4, 8, 128, 128),
        (4, 4, 8, 2, 16, 128), (4, 4, 8, 2, 16, 128), (8, 512, 128), (8, 4, 128, 128),
    ]
    scratch = [pltpu.VMEM(shape, F32) for shape in half]
    scratch += [pltpu.VMEM((512, 512), F32)] * 3
    scratch += [pltpu.VMEM((1536, 512), BF)] * 2 + [pltpu.VMEM((512, 1536), BF)] * 3 + [pltpu.VMEM((4, 512, 384), BF)]
    scratch += [pltpu.VMEM((256, 1536), BF), pltpu.VMEM((1536, 256), BF)]
    scratch += [pltpu.VMEM((8, 1024, 256), BF), pltpu.VMEM((512, 128), F32)]
    dma = pltpu.SemaphoreType.DMA
    scratch += [dma((3,)), dma((12,))] + [dma((STEPS,))] * 4
    scratch += [dma((STEPS,))] * 6 + [dma((2,))]
    whole = pl.BlockSpec(memory_space=pl.ANY)
    vmem = pl.BlockSpec(memory_space=pltpu.VMEM)
    smem = pl.BlockSpec(memory_space=pltpu.SMEM)
    return pl.pallas_call(
        kernel,
        out_shape=pltpu.VMEM((64, 128, 128), F32),
        in_specs=[whole, whole, whole, whole, vmem, smem, vmem, smem],
        out_specs=vmem,
        scratch_shapes=scratch,
        compiler_params=pltpu.CompilerParams(
            collective_id=0, has_side_effects=True, vmem_limit_bytes=62500000
        ),
        name="kron_solve",
    )(
        targets, basis_first, basis_second, basis_third,
        eigen_first.reshape(1, 512), eigen_second, eigen_third.reshape(4, 128), noise,
    )


def solution(mesh):
    in_specs = (P("gx", "gy", "gz"), P(), P(), P(), P(), P(), P(), P())
    return jax.shard_map(
        per_device, mesh=mesh, in_specs=in_specs, out_specs=P("gx", "gy", "gz"), check_vma=False
    )
```

```python
import functools

import jax
import jax.numpy as jnp
from jax import lax
from jax.experimental import pallas as pl
from jax.experimental.pallas import tpu as pltpu
from jax.sharding import PartitionSpec as P

MESH = pl.DeviceIdType.MESH
BF = jnp.bfloat16
F32 = jnp.float32
STEPS = 4
DEPTH = 512
ORDER = ("q|e", "eq", "eq", "eq")


def halves(value):
    high = value.astype(BF)
    return high, (value - high.astype(F32)).astype(BF)


def kernel(
    t_ref, b1_ref, b2_ref, b3_ref, e1_ref, e2_ref, e3_ref, noise_ref, o_ref,
    re1, se2, re2, se3, rq1, sq2, rq2, sq3, r3, s3,
    re3p, se2p, re2p, se1p, rq3p, sq2p, rq2p, sq1p,
    b1f, b2f, b3f, b3c, b3tc, b2l, b2tl, b1l, b1tm, lhs, rhs, mid, e1b,
    base_sem, send, in_e1, in_q1, in_e2, in_q2, in_me, in_mq, in_e3p, in_q3p, in_e2p, in_q2p, in_out,
):
    w, x, q = lax.axis_index("gx"), lax.axis_index("gy"), lax.axis_index("gz")
    y, z, core = w // 2, (q // 2) * 2 + w % 2, q % 2
    beta = w * 4 + q

    def far(dy, dz, dc):
        y2, z2, c2 = (y + dy) % 4, (z + dz) % 4, (core + dc) % 2
        return y2 * 2 + z2 % 2, (z2 // 2) * 2 + c2

    def each_far(act):
        def both(n, _):
            k = n // 2
            act(*far(k % 3 + 1, (k % 3 + k // 3) % 3 + 1, n % 2))
            return _

        def one(n, _):
            act(*far(n // 2 + 1, 0, n % 2))
            return _

        def other(n, _):
            act(*far(0, n // 2 + 1, n % 2))
            return _

        lax.fori_loop(0, 18, both, 0)
        lax.fori_loop(0, 6, one, 0)
        lax.fori_loop(0, 6, other, 0)
        act(*far(0, 0, 1))

    def push(src, dst, sem, arrival, where):
        pltpu.make_async_remote_copy(
            src_ref=src, dst_ref=dst, send_sem=send.at[sem], recv_sem=arrival,
            device_id=where, device_id_type=MESH,
        ).start()

    def await_bytes(ref, sem):
        pltpu.make_async_copy(ref, ref, sem).wait()

    def staged(part_e, part_q, orders):
        for order in orders.split("|"):
            def body(s, _):
                for part in order:
                    (part_e if part == "e" else part_q)(s)
                return _

            lax.fori_loop(0, STEPS, body, 0)

    loads = [
        pltpu.make_async_copy(ref, buf, base_sem.at[n])
        for n, (ref, buf) in enumerate(((b3_ref, b3f), (b2_ref, b2f), (b1_ref, b1f)))
    ]
    for load in loads:
        load.start()

    barrier = pltpu.get_barrier_semaphore()

    def greet(w2, q2):
        pl.semaphore_signal(barrier, inc=1, device_id=(w2, x, q2), device_id_type=MESH)

    for d in (1, 2, 3):
        pl.semaphore_signal(barrier, inc=1, device_id=(w, (x + d) % 4, q), device_id_type=MESH)
    each_far(greet)
    pl.semaphore_wait(barrier, 34)

    def first(s, _):
        two = pl.ds(s * 2, 2)
        for d in (2, 1, 3):
            q2, x2 = (q + d) % 4, (x + d) % 4
            push(t_ref.at[pl.ds(q2 * 8 + s * 2, 2)], re1.at[q, two], 0, in_e1.at[s], (w, x, q2))
            push(t_ref.at[pl.ds(32 + x2 * 8 + s * 2, 2)], rq1.at[two, x], 1, in_q1.at[s], (w, x2, q))
        pltpu.make_async_copy(t_ref.at[pl.ds(q * 8 + s * 2, 2)], re1.at[q, two], in_e1.at[s]).start()
        pltpu.make_async_copy(t_ref.at[pl.ds(32 + x * 8 + s * 2, 2)], rq1.at[two, x], in_q1.at[s]).start()
        return _

    lax.fori_loop(0, STEPS, first, 0)

    def columns(target, value):
        high, low = halves(value)
        target[0:512, :] = high
        target[512:1024, :] = low
        target[1024:1536, :] = high

    def rows(target, value):
        high, low = halves(value)
        target[:, 0:512] = high
        target[:, 512:1024] = high
        target[:, 1024:1536] = low

    loads[0].wait()
    columns(b3c, b3f[...])
    loads[1].wait()
    rows(b2tl, b2f[...].T)

    def data_left(piece, factor):
        for k in range(4):
            high, low = halves(piece(k))
            lhs[:, k * 128 : k * 128 + 128] = high
            lhs[:, 512 + k * 128 : 640 + k * 128] = high
            lhs[:, 1024 + k * 128 : 1152 + k * 128] = low
        return jnp.dot(lhs[...], factor[...], preferred_element_type=F32)

    def data_right(factor, piece):
        for k in range(2):
            high, low = halves(piece(k))
            lanes = slice(k * 128, k * 128 + 128)
            rhs[0:512, lanes] = high
            rhs[512:1024, lanes] = low
            rhs[1024:1536, lanes] = high
        return jnp.dot(factor[...], rhs[...], preferred_element_type=F32)

    def stage_one_e(s):
        two = pl.ds(s * 2, 2)
        await_bytes(re1.at[:, two], in_e1.at[s])
        out = data_left(lambda k: re1[k, two].reshape(256, 128), b3c)
        for n in range(4):
            se2[n, two] = out[:, n * 128 : n * 128 + 128].reshape(2, 128, 128)
        for d in (2, 1, 3):
            x2 = (x + d) % 4
            push(se2.at[x2, two], re2.at[two, x], 2, in_e2.at[s], (w, x2, q))
        re2[two, x] = se2[x, two]

    def stage_one_q(s):
        two = pl.ds(s * 2, 2)
        await_bytes(rq1.at[two], in_q1.at[s])
        out = data_right(b2tl, lambda k: rq1[s * 2 + k].reshape(512, 128))
        sq2[s * 2] = out[:, 0:128]
        sq2[s * 2 + 1] = out[:, 128:256]

        def spread(w2, q2):
            push(
                sq2.at[two, pl.ds((w2 * 4 + q2) * 16, 16)], rq2.at[q, w, two],
                3, in_q2.at[s], (w2, x, q2),
            )

        each_far(spread)
        rq2[q, w, two] = sq2[two, pl.ds(pl.multiple_of(beta * 16, 16), 16)]

    staged(stage_one_e, stage_one_q, ORDER[0])

    loads[2].wait()
    place = lax.broadcasted_iota(jnp.int32, (DEPTH, DEPTH), 0)
    source = (place % 128) // 2 * 8 + place // 128 * 2 + place % 2
    pick = (lax.broadcasted_iota(jnp.int32, (DEPTH, DEPTH), 1) == source).astype(F32).astype(BF)
    high, low = halves(b1f[...])
    high = jnp.dot(pick, high, preferred_element_type=F32)
    low = jnp.dot(pick, low, preferred_element_type=F32)
    b1l[:, 0:512] = high.astype(BF)
    b1l[:, 512:1024] = high.astype(BF)
    b1l[:, 1024:1536] = low.astype(BF)
    high, low = high.T.astype(BF), low.T.astype(BF)
    for n in range(STEPS):
        b1tm[n, :, 0:128] = high[:, n * 128 : n * 128 + 128]
        b1tm[n, :, 128:256] = high[:, n * 128 : n * 128 + 128]
        b1tm[n, :, 256:384] = low[:, n * 128 : n * 128 + 128]
    s3[...] = jnp.zeros_like(s3)
    e1b[...] = jnp.broadcast_to(e1_ref[...], (128, DEPTH)).T
    along = e3_ref[pl.ds(x, 1), :]
    inverse = (se1p.reshape(4096, 128), sq1p.reshape(4096, 128))

    def column(at):
        return pl.ds(pl.multiple_of(at * DEPTH, DEPTH), DEPTH)

    def invert(pair, _):
        for k in range(2):
            spectrum = e1b[...] * e2_ref[beta * 16 + pair * 2 + k] * along + noise_ref[0]
            inverse[k][column(pair), :] = 1.0 / spectrum
        return _

    lax.fori_loop(0, 8, invert, 0)

    def stage_two_e(s):
        two = pl.ds(s * 2, 2)
        await_bytes(re2.at[two, pl.ds(0, 3)], in_e2.at[s])
        out = data_right(b2tl, lambda k: re2[s * 2 + k].reshape(512, 128))
        se3[s * 2] = out[:, 0:128]
        se3[s * 2 + 1] = out[:, 128:256]

        def spread(w2, q2):
            push(
                se3.at[two, pl.ds((w2 * 4 + q2) * 16, 16)], r3.at[s, w, 0, q],
                4, in_me.at[s], (w2, x, q2),
            )

        each_far(spread)
        r3[s, w, 0, q] = se3[two, pl.ds(pl.multiple_of(beta * 16, 16), 16)]

    def stage_two_q(s):
        two = pl.ds(s * 2, 2)
        await_bytes(sq2.at[pl.ds(0, 2), pl.ds(0, 496)], in_q2.at[s])
        out = data_left(lambda k: rq2[k, :, two].reshape(256, 128), b3c)
        for n in range(4):
            sq3[n, :, two] = out[:, n * 128 : n * 128 + 128].reshape(8, 2, 16, 128)
        for d in (2, 1, 3):
            x2 = (x + d) % 4
            push(sq3.at[x2, :, two], r3.at[s, :, 1, x], 5, in_mq.at[s], (w, x2, q))
        r3[s, :, 1, x] = sq3[x, :, two]

    staged(stage_two_e, stage_two_q, ORDER[1])

    rows(b2l, b2f[...])
    columns(b3tc, b3f[...].T)

    flat = r3.reshape(8192, 128)
    flat_s = s3.reshape(8192, 128)
    def arrived(s):
        await_bytes(se3.at[pl.ds(0, 2), pl.ds(0, 496)], in_me.at[s])
        await_bytes(sq3.at[pl.ds(0, 3), :, pl.ds(0, 2)], in_mq.at[s])

    def term(s, pair):
        for k in range(2):
            high, low = halves(flat[pl.ds(s * 2048 + pair * 2 + k, 128, stride=16), :])
            lanes = slice(k * 128, k * 128 + 128)
            rhs[0:128, lanes] = high
            rhs[128:256, lanes] = low
            rhs[256:384, lanes] = high
        return jnp.dot(b1tm[s], rhs[0:384, :], preferred_element_type=F32)

    def total(at):
        return flat_s.at[column(at), :]

    def gather_sum(s, _):
        arrived(s)

        def one_pair(pair, _):
            part = term(s, pair)
            for k in range(2):
                total(pair * 2 + k)[...] += part[:, k * 128 : k * 128 + 128]
            return _

        lax.fori_loop(0, 8, one_pair, 0)
        return _

    lax.fori_loop(0, STEPS - 1, gather_sum, 0)
    arrived(STEPS - 1)

    def middle(pair, _):
        part = term(STEPS - 1, pair)
        for k in range(2):
            at = pair * 2 + k
            lanes = slice(k * 128, k * 128 + 128)
            high, low = halves((total(at)[...] + part[:, lanes]) * inverse[k][column(pair), :])
            mid[pair, 0:512, lanes] = high
            mid[pair, 512:1024, lanes] = low
        return _

    lax.fori_loop(0, 8, middle, 0)

    def back_mid(s, _):
        factor = b1l[pl.ds(pl.multiple_of(s * 128, 128), 128), :]
        for pair in range(8):
            out = jnp.dot(factor[:, 0:1024], mid[pair], preferred_element_type=F32)
            out += jnp.dot(factor[:, 1024:1536], mid[pair, 0:512], preferred_element_type=F32)
            for k in range(2):
                flat_s[pl.ds(s * 2048 + pair * 2 + k, 128, stride=16), :] = out[:, k * 128 : k * 128 + 128]
        for d in (2, 1, 3):
            x2 = (x + d) % 4
            push(s3.at[s, :, 1, x2], rq3p.at[x, s], 6, in_q3p.at[s], (w, x2, q))

        def spread(w2, q2):
            push(
                s3.at[s, w2, 0, q2],
                re3p.at[pl.ds(s * 2, 2), pl.ds(pl.multiple_of(beta * 16, 16), 16)],
                7, in_e3p.at[s], (w2, x, q2),
            )

        each_far(spread)
        rq3p[x, s] = s3[s, :, 1, x]
        re3p[pl.ds(s * 2, 2), pl.ds(pl.multiple_of(beta * 16, 16), 16)] = s3[s, w, 0, q]
        return _

    lax.fori_loop(0, STEPS, back_mid, 0)

    def back_one_e(s):
        two = pl.ds(s * 2, 2)
        await_bytes(se3.at[pl.ds(0, 2), pl.ds(0, 496)], in_e3p.at[s])
        out = data_right(b2l, lambda k: re3p[s * 2 + k])
        for k in range(2):
            se2p[s * 2 + k] = out[:, k * 128 : k * 128 + 128].reshape(4, 128, 128)
        for d in (2, 1, 3):
            x2 = (x + d) % 4
            push(se2p.at[two, x2], re2p.at[x, two], 9, in_e2p.at[s], (w, x2, q))
        re2p[x, two] = se2p[two, x]

    def back_one_q(s):
        two = pl.ds(s * 2, 2)
        await_bytes(rq3p.at[pl.ds(0, 3), s], in_q3p.at[s])
        out = data_left(lambda k: rq3p[k, s].reshape(256, 128), b3tc)
        for n in range(4):
            sq2p[n, s] = out[:, n * 128 : n * 128 + 128].reshape(8, 2, 16, 128)

        def spread(w2, q2):
            push(
                sq2p.at[q2, s, w2],
                rq2p.at[two, pl.ds(pl.multiple_of(beta * 16, 16), 16)],
                8, in_q2p.at[s], (w2, x, q2),
            )

        each_far(spread)
        rq2p[two, pl.ds(pl.multiple_of(beta * 16, 16), 16)] = sq2p[q, s, w]

    staged(back_one_e, back_one_q, ORDER[2])

    def back_two_e(s):
        two = pl.ds(s * 2, 2)
        await_bytes(re2p.at[pl.ds(0, 3), two], in_e2p.at[s])
        out = data_left(lambda k: re2p[k, two].reshape(256, 128), b3tc)
        for n in range(4):
            se1p[n, two] = out[:, n * 128 : n * 128 + 128].reshape(2, 128, 128)
        here = o_ref.at[pl.ds(q * 8 + s * 2, 2)]
        for d in (2, 1, 3):
            q2 = (q + d) % 4
            push(se1p.at[q2, two], here, 10, in_out.at[0], (w, x, q2))
        pltpu.make_async_copy(se1p.at[q, two], here, in_out.at[0]).start()

    def back_two_q(s):
        two = pl.ds(s * 2, 2)
        await_bytes(se3.at[pl.ds(0, 2), pl.ds(0, 496)], in_q2p.at[s])
        out = data_right(b2l, lambda k: rq2p[s * 2 + k])
        for k in range(2):
            sq1p[s * 2 + k] = out[:, k * 128 : k * 128 + 128].reshape(4, 128, 128)
        here = o_ref.at[pl.ds(32 + x * 8 + s * 2, 2)]
        for d in (2, 1, 3):
            x2 = (x + d) % 4
            push(sq1p.at[two, x2], here, 11, in_out.at[1], (w, x2, q))
        pltpu.make_async_copy(sq1p.at[two, x], here, in_out.at[1]).start()

    staged(back_two_e, back_two_q, ORDER[3])

    await_bytes(re1, in_out.at[0])
    await_bytes(re1, in_out.at[1])
    for sem in (0, 1, 2, 5, 6, 9, 10, 11):
        await_bytes(re1.at[pl.ds(0, 3)], send.at[sem])
    for sem in (3, 4, 7, 8):
        await_bytes(se3.at[:, pl.ds(0, 496)], send.at[sem])


def per_device(targets, basis_first, basis_second, basis_third, eigen_first, eigen_second, eigen_third, noise):
    half = [
        (4, 8, 128, 128), (4, 8, 128, 128), (8, 4, 128, 128), (8, 512, 128),
        (8, 4, 128, 128), (8, 512, 128), (4, 8, 8, 16, 128), (4, 8, 8, 16, 128),
        (4, 8, 2, 4, 2, 16, 128), (4, 8, 2, 4, 2, 16, 128),
        (8, 512, 128), (8, 4, 128, 128), (4, 8, 128, 128), (4, 8, 128, 128),
        (4, 4, 8, 2, 16, 128), (4, 4, 8, 2, 16, 128), (8, 512, 128), (8, 4, 128, 128),
    ]
    scratch = [pltpu.VMEM(shape, F32) for shape in half]
    scratch += [pltpu.VMEM((512, 512), F32)] * 3
    scratch += [pltpu.VMEM((1536, 512), BF)] * 2 + [pltpu.VMEM((512, 1536), BF)] * 3 + [pltpu.VMEM((4, 512, 384), BF)]
    scratch += [pltpu.VMEM((256, 1536), BF), pltpu.VMEM((1536, 256), BF)]
    scratch += [pltpu.VMEM((8, 1024, 256), BF), pltpu.VMEM((512, 128), F32)]
    dma = pltpu.SemaphoreType.DMA
    scratch += [dma((3,)), dma((12,))] + [dma((STEPS,))] * 4
    scratch += [dma((STEPS,))] * 6 + [dma((2,))]
    whole = pl.BlockSpec(memory_space=pl.ANY)
    vmem = pl.BlockSpec(memory_space=pltpu.VMEM)
    smem = pl.BlockSpec(memory_space=pltpu.SMEM)
    return pl.pallas_call(
        kernel,
        out_shape=pltpu.VMEM((64, 128, 128), F32),
        in_specs=[whole, whole, whole, whole, vmem, smem, vmem, smem],
        out_specs=vmem,
        scratch_shapes=scratch,
        compiler_params=pltpu.CompilerParams(
            collective_id=0, has_side_effects=True, vmem_limit_bytes=62500000
        ),
        name="kron_solve",
    )(
        targets, basis_first, basis_second, basis_third,
        eigen_first.reshape(1, 512), eigen_second, eigen_third.reshape(4, 128), noise,
    )


def solution(mesh):
    in_specs = (P("gx", "gy", "gz"), P(), P(), P(), P(), P(), P(), P())
    return jax.shard_map(
        per_device, mesh=mesh, in_specs=in_specs, out_specs=P("gx", "gy", "gz"), check_vma=False
    )
```

```python
import functools

import jax
import jax.numpy as jnp
from jax import lax
from jax.experimental import pallas as pl
from jax.experimental.pallas import tpu as pltpu
from jax.sharding import PartitionSpec as P

MESH = pl.DeviceIdType.MESH
BF = jnp.bfloat16
F32 = jnp.float32
STEPS = 4
DEPTH = 512
ORDER = ("q|e", "eq", "eq", "eq")


def halves(value):
    high = value.astype(BF)
    return high, (value - high.astype(F32)).astype(BF)


def kernel(
    t_ref, b1_ref, b2_ref, b3_ref, e1_ref, e2_ref, e3_ref, noise_ref, o_ref,
    re1, se2, re2, se3, rq1, sq2, rq2, sq3, r3, s3,
    re3p, se2p, re2p, se1p, rq3p, sq2p, rq2p, sq1p,
    b1f, b2f, b3f, b3c, b3tc, b2l, b2tl, b1l, b1tm, lhs, rhs, mid, e1b,
    base_sem, send, in_e1, in_q1, in_e2, in_q2, in_me, in_mq, in_e3p, in_q3p, in_e2p, in_q2p, in_out,
):
    w, x, q = lax.axis_index("gx"), lax.axis_index("gy"), lax.axis_index("gz")
    y, z, core = w // 2, (q // 2) * 2 + w % 2, q % 2
    beta = w * 4 + q

    def far(dy, dz, dc):
        y2, z2, c2 = (y + dy) % 4, (z + dz) % 4, (core + dc) % 2
        return y2 * 2 + z2 % 2, (z2 // 2) * 2 + c2

    def each_far(act):
        def both(n, _):
            k = n // 2
            act(*far(k % 3 + 1, (k % 3 + k // 3) % 3 + 1, n % 2))
            return _

        def one(n, _):
            act(*far(n // 2 + 1, 0, n % 2))
            return _

        def other(n, _):
            act(*far(0, n // 2 + 1, n % 2))
            return _

        lax.fori_loop(0, 18, both, 0)
        lax.fori_loop(0, 6, one, 0)
        lax.fori_loop(0, 6, other, 0)
        act(*far(0, 0, 1))

    def push(src, dst, sem, arrival, where):
        pltpu.make_async_remote_copy(
            src_ref=src, dst_ref=dst, send_sem=send.at[sem], recv_sem=arrival,
            device_id=where, device_id_type=MESH,
        ).start()

    def await_bytes(ref, sem):
        pltpu.make_async_copy(ref, ref, sem).wait()

    def staged(part_e, part_q, orders):
        for order in orders.split("|"):
            def body(s, _):
                for part in order:
                    (part_e if part == "e" else part_q)(s)
                return _

            lax.fori_loop(0, STEPS, body, 0)

    loads = [
        pltpu.make_async_copy(ref, buf, base_sem.at[n])
        for n, (ref, buf) in enumerate(((b3_ref, b3f), (b2_ref, b2f), (b1_ref, b1f)))
    ]
    for load in loads:
        load.start()

    barrier = pltpu.get_barrier_semaphore()

    def greet(w2, q2):
        pl.semaphore_signal(barrier, inc=1, device_id=(w2, x, q2), device_id_type=MESH)

    for d in (1, 2, 3):
        pl.semaphore_signal(barrier, inc=1, device_id=(w, (x + d) % 4, q), device_id_type=MESH)
    each_far(greet)
    pl.semaphore_wait(barrier, 34)

    def first(s, _):
        two = pl.ds(s * 2, 2)
        for d in (2, 1, 3):
            q2, x2 = (q + d) % 4, (x + d) % 4
            push(t_ref.at[pl.ds(q2 * 8 + s * 2, 2)], re1.at[q, two], 0, in_e1.at[s], (w, x, q2))
            push(t_ref.at[pl.ds(32 + x2 * 8 + s * 2, 2)], rq1.at[two, x], 1, in_q1.at[s], (w, x2, q))
        pltpu.make_async_copy(t_ref.at[pl.ds(q * 8 + s * 2, 2)], re1.at[q, two], in_e1.at[s]).start()
        pltpu.make_async_copy(t_ref.at[pl.ds(32 + x * 8 + s * 2, 2)], rq1.at[two, x], in_q1.at[s]).start()
        return _

    lax.fori_loop(0, STEPS, first, 0)

    def columns(target, value):
        high, low = halves(value)
        target[0:512, :] = high
        target[512:1024, :] = low
        target[1024:1536, :] = high

    def rows(target, value):
        high, low = halves(value)
        target[:, 0:512] = high
        target[:, 512:1024] = high
        target[:, 1024:1536] = low

    loads[0].wait()
    columns(b3c, b3f[...])
    loads[1].wait()
    rows(b2tl, b2f[...].T)

    def data_left(piece, factor):
        for k in range(4):
            high, low = halves(piece(k))
            lhs[:, k * 128 : k * 128 + 128] = high
            lhs[:, 512 + k * 128 : 640 + k * 128] = high
            lhs[:, 1024 + k * 128 : 1152 + k * 128] = low
        return jnp.dot(lhs[...], factor[...], preferred_element_type=F32)

    def data_right(factor, piece):
        for k in range(2):
            high, low = halves(piece(k))
            lanes = slice(k * 128, k * 128 + 128)
            rhs[0:512, lanes] = high
            rhs[512:1024, lanes] = low
            rhs[1024:1536, lanes] = high
        return jnp.dot(factor[...], rhs[...], preferred_element_type=F32)

    def stage_one_e(s):
        two = pl.ds(s * 2, 2)
        await_bytes(re1.at[:, two], in_e1.at[s])
        out = data_left(lambda k: re1[k, two].reshape(256, 128), b3c)
        for n in range(4):
            se2[n, two] = out[:, n * 128 : n * 128 + 128].reshape(2, 128, 128)
        for d in (2, 1, 3):
            x2 = (x + d) % 4
            push(se2.at[x2, two], re2.at[two, x], 2, in_e2.at[s], (w, x2, q))
        re2[two, x] = se2[x, two]

    def stage_one_q(s):
        two = pl.ds(s * 2, 2)
        await_bytes(rq1.at[two], in_q1.at[s])
        out = data_right(b2tl, lambda k: rq1[s * 2 + k].reshape(512, 128))
        sq2[s * 2] = out[:, 0:128]
        sq2[s * 2 + 1] = out[:, 128:256]

        def spread(w2, q2):
            push(
                sq2.at[two, pl.ds((w2 * 4 + q2) * 16, 16)], rq2.at[q, w, two],
                3, in_q2.at[s], (w2, x, q2),
            )

        each_far(spread)
        rq2[q, w, two] = sq2[two, pl.ds(pl.multiple_of(beta * 16, 16), 16)]

    staged(stage_one_e, stage_one_q, ORDER[0])

    loads[2].wait()
    place = lax.broadcasted_iota(jnp.int32, (DEPTH, DEPTH), 0)
    source = (place % 128) // 2 * 8 + place // 128 * 2 + place % 2
    pick = (lax.broadcasted_iota(jnp.int32, (DEPTH, DEPTH), 1) == source).astype(F32).astype(BF)
    high, low = halves(b1f[...])
    high = jnp.dot(pick, high, preferred_element_type=F32)
    low = jnp.dot(pick, low, preferred_element_type=F32)
    b1l[:, 0:512] = high.astype(BF)
    b1l[:, 512:1024] = high.astype(BF)
    b1l[:, 1024:1536] = low.astype(BF)
    high, low = high.T.astype(BF), low.T.astype(BF)
    for n in range(STEPS):
        b1tm[n, :, 0:128] = high[:, n * 128 : n * 128 + 128]
        b1tm[n, :, 128:256] = high[:, n * 128 : n * 128 + 128]
        b1tm[n, :, 256:384] = low[:, n * 128 : n * 128 + 128]
    s3[...] = jnp.zeros_like(s3)
    e1b[...] = jnp.broadcast_to(e1_ref[...], (128, DEPTH)).T
    along = e3_ref[pl.ds(x, 1), :]
    inverse = (se1p.reshape(4096, 128), sq1p.reshape(4096, 128))

    def column(at):
        return pl.ds(pl.multiple_of(at * DEPTH, DEPTH), DEPTH)

    def invert(pair, _):
        for k in range(2):
            spectrum = e1b[...] * e2_ref[beta * 16 + pair * 2 + k] * along + noise_ref[0]
            inverse[k][column(pair), :] = 1.0 / spectrum
        return _

    lax.fori_loop(0, 8, invert, 0)

    def stage_two_e(s):
        two = pl.ds(s * 2, 2)
        await_bytes(re2.at[two, pl.ds(0, 3)], in_e2.at[s])
        out = data_right(b2tl, lambda k: re2[s * 2 + k].reshape(512, 128))
        se3[s * 2] = out[:, 0:128]
        se3[s * 2 + 1] = out[:, 128:256]

        def spread(w2, q2):
            push(
                se3.at[two, pl.ds((w2 * 4 + q2) * 16, 16)], r3.at[s, w, 0, q],
                4, in_me.at[s], (w2, x, q2),
            )

        each_far(spread)
        r3[s, w, 0, q] = se3[two, pl.ds(pl.multiple_of(beta * 16, 16), 16)]

    def stage_two_q(s):
        two = pl.ds(s * 2, 2)
        await_bytes(sq2.at[pl.ds(0, 2), pl.ds(0, 496)], in_q2.at[s])
        out = data_left(lambda k: rq2[k, :, two].reshape(256, 128), b3c)
        for n in range(4):
            sq3[n, :, two] = out[:, n * 128 : n * 128 + 128].reshape(8, 2, 16, 128)
        for d in (2, 1, 3):
            x2 = (x + d) % 4
            push(sq3.at[x2, :, two], r3.at[s, :, 1, x], 5, in_mq.at[s], (w, x2, q))
        r3[s, :, 1, x] = sq3[x, :, two]

    staged(stage_two_e, stage_two_q, ORDER[1])

    rows(b2l, b2f[...])
    columns(b3tc, b3f[...].T)

    flat = r3.reshape(8192, 128)
    flat_s = s3.reshape(8192, 128)
    def arrived(s):
        await_bytes(se3.at[pl.ds(0, 2), pl.ds(0, 496)], in_me.at[s])
        await_bytes(sq3.at[pl.ds(0, 3), :, pl.ds(0, 2)], in_mq.at[s])

    def term(s, pair):
        for k in range(2):
            high, low = halves(flat[pl.ds(s * 2048 + pair * 2 + k, 128, stride=16), :])
            lanes = slice(k * 128, k * 128 + 128)
            rhs[0:128, lanes] = high
            rhs[128:256, lanes] = low
            rhs[256:384, lanes] = high
        return jnp.dot(b1tm[s], rhs[0:384, :], preferred_element_type=F32)

    def total(at):
        return flat_s.at[column(at), :]

    def gather_sum(s, _):
        arrived(s)

        def one_pair(pair, _):
            part = term(s, pair)
            for k in range(2):
                total(pair * 2 + k)[...] += part[:, k * 128 : k * 128 + 128]
            return _

        lax.fori_loop(0, 8, one_pair, 0)
        return _

    lax.fori_loop(0, STEPS - 1, gather_sum, 0)
    arrived(STEPS - 1)

    def middle(pair, _):
        part = term(STEPS - 1, pair)
        for k in range(2):
            at = pair * 2 + k
            lanes = slice(k * 128, k * 128 + 128)
            high, low = halves((total(at)[...] + part[:, lanes]) * inverse[k][column(pair), :])
            mid[pair, 0:512, lanes] = high
            mid[pair, 512:1024, lanes] = low
        return _

    def turn(s, pair):
        factor = b1l[pl.ds(pl.multiple_of(s * 128, 128), 128), :]
        out = jnp.dot(factor[:, 0:1024], mid[pair], preferred_element_type=F32)
        out += jnp.dot(factor[:, 1024:1536], mid[pair, 0:512], preferred_element_type=F32)
        for k in range(2):
            flat_s[pl.ds(s * 2048 + pair * 2 + k, 128, stride=16), :] = out[:, k * 128 : k * 128 + 128]

    def send_back(s, low, count):
        some = pl.ds(low, count)
        mine = pl.ds(pl.multiple_of(beta * 16 + low, 8), count)
        two = pl.ds(s * 2, 2)
        for d in (2, 1, 3):
            x2 = (x + d) % 4
            push(s3.at[s, :, 1, x2, :, some], rq3p.at[x, s, :, :, some], 6, in_q3p.at[s], (w, x2, q))

        def spread(w2, q2):
            push(s3.at[s, w2, 0, q2, :, some], re3p.at[two, mine], 7, in_e3p.at[s], (w2, x, q2))

        each_far(spread)
        rq3p[x, s, :, :, some] = s3[s, :, 1, x, :, some]
        re3p[two, mine] = s3[s, w, 0, q, :, some]

    for part in range(2):
        lax.fori_loop(part * 4, part * 4 + 4, middle, 0)
        for pair in range(part * 4, part * 4 + 4):
            turn(0, pair)
        send_back(0, part * 8, 8)

    def back_mid(s, _):
        for pair in range(8):
            turn(s, pair)
        send_back(s, 0, 16)
        return _

    lax.fori_loop(1, STEPS, back_mid, 0)

    def back_one_e(s):
        two = pl.ds(s * 2, 2)
        await_bytes(se3.at[pl.ds(0, 2), pl.ds(0, 496)], in_e3p.at[s])
        out = data_right(b2l, lambda k: re3p[s * 2 + k])
        for k in range(2):
            se2p[s * 2 + k] = out[:, k * 128 : k * 128 + 128].reshape(4, 128, 128)
        for d in (2, 1, 3):
            x2 = (x + d) % 4
            push(se2p.at[two, x2], re2p.at[x, two], 9, in_e2p.at[s], (w, x2, q))
        re2p[x, two] = se2p[two, x]

    def back_one_q(s):
        two = pl.ds(s * 2, 2)
        await_bytes(rq3p.at[pl.ds(0, 3), s], in_q3p.at[s])
        out = data_left(lambda k: rq3p[k, s].reshape(256, 128), b3tc)
        for n in range(4):
            sq2p[n, s] = out[:, n * 128 : n * 128 + 128].reshape(8, 2, 16, 128)

        def spread(w2, q2):
            push(
                sq2p.at[q2, s, w2],
                rq2p.at[two, pl.ds(pl.multiple_of(beta * 16, 16), 16)],
                8, in_q2p.at[s], (w2, x, q2),
            )

        each_far(spread)
        rq2p[two, pl.ds(pl.multiple_of(beta * 16, 16), 16)] = sq2p[q, s, w]

    staged(back_one_e, back_one_q, ORDER[2])

    def back_two_e(s):
        two = pl.ds(s * 2, 2)
        await_bytes(re2p.at[pl.ds(0, 3), two], in_e2p.at[s])
        out = data_left(lambda k: re2p[k, two].reshape(256, 128), b3tc)
        for n in range(4):
            se1p[n, two] = out[:, n * 128 : n * 128 + 128].reshape(2, 128, 128)
        here = o_ref.at[pl.ds(q * 8 + s * 2, 2)]
        for d in (2, 1, 3):
            q2 = (q + d) % 4
            push(se1p.at[q2, two], here, 10, in_out.at[0], (w, x, q2))
        pltpu.make_async_copy(se1p.at[q, two], here, in_out.at[0]).start()

    def back_two_q(s):
        two = pl.ds(s * 2, 2)
        await_bytes(se3.at[pl.ds(0, 2), pl.ds(0, 496)], in_q2p.at[s])
        out = data_right(b2l, lambda k: rq2p[s * 2 + k])
        for k in range(2):
            sq1p[s * 2 + k] = out[:, k * 128 : k * 128 + 128].reshape(4, 128, 128)
        here = o_ref.at[pl.ds(32 + x * 8 + s * 2, 2)]
        for d in (2, 1, 3):
            x2 = (x + d) % 4
            push(sq1p.at[two, x2], here, 11, in_out.at[1], (w, x2, q))
        pltpu.make_async_copy(sq1p.at[two, x], here, in_out.at[1]).start()

    staged(back_two_e, back_two_q, ORDER[3])

    await_bytes(re1, in_out.at[0])
    await_bytes(re1, in_out.at[1])
    for sem in (0, 1, 2, 5, 6, 9, 10, 11):
        await_bytes(re1.at[pl.ds(0, 3)], send.at[sem])
    for sem in (3, 4, 7, 8):
        await_bytes(se3.at[:, pl.ds(0, 496)], send.at[sem])


def per_device(targets, basis_first, basis_second, basis_third, eigen_first, eigen_second, eigen_third, noise):
    half = [
        (4, 8, 128, 128), (4, 8, 128, 128), (8, 4, 128, 128), (8, 512, 128),
        (8, 4, 128, 128), (8, 512, 128), (4, 8, 8, 16, 128), (4, 8, 8, 16, 128),
        (4, 8, 2, 4, 2, 16, 128), (4, 8, 2, 4, 2, 16, 128),
        (8, 512, 128), (8, 4, 128, 128), (4, 8, 128, 128), (4, 8, 128, 128),
        (4, 4, 8, 2, 16, 128), (4, 4, 8, 2, 16, 128), (8, 512, 128), (8, 4, 128, 128),
    ]
    scratch = [pltpu.VMEM(shape, F32) for shape in half]
    scratch += [pltpu.VMEM((512, 512), F32)] * 3
    scratch += [pltpu.VMEM((1536, 512), BF)] * 2 + [pltpu.VMEM((512, 1536), BF)] * 3 + [pltpu.VMEM((4, 512, 384), BF)]
    scratch += [pltpu.VMEM((256, 1536), BF), pltpu.VMEM((1536, 256), BF)]
    scratch += [pltpu.VMEM((8, 1024, 256), BF), pltpu.VMEM((512, 128), F32)]
    dma = pltpu.SemaphoreType.DMA
    scratch += [dma((3,)), dma((12,))] + [dma((STEPS,))] * 4
    scratch += [dma((STEPS,))] * 6 + [dma((2,))]
    whole = pl.BlockSpec(memory_space=pl.ANY)
    vmem = pl.BlockSpec(memory_space=pltpu.VMEM)
    smem = pl.BlockSpec(memory_space=pltpu.SMEM)
    return pl.pallas_call(
        kernel,
        out_shape=pltpu.VMEM((64, 128, 128), F32),
        in_specs=[whole, whole, whole, whole, vmem, smem, vmem, smem],
        out_specs=vmem,
        scratch_shapes=scratch,
        compiler_params=pltpu.CompilerParams(
            collective_id=0, has_side_effects=True, vmem_limit_bytes=62500000
        ),
        name="kron_solve",
    )(
        targets, basis_first, basis_second, basis_third,
        eigen_first.reshape(1, 512), eigen_second, eigen_third.reshape(4, 128), noise,
    )


def solution(mesh):
    in_specs = (P("gx", "gy", "gz"), P(), P(), P(), P(), P(), P(), P())
    return jax.shard_map(
        per_device, mesh=mesh, in_specs=in_specs, out_specs=P("gx", "gy", "gz"), check_vma=False
    )
```

```python
import functools

import jax
import jax.numpy as jnp
from jax import lax
from jax.experimental import pallas as pl
from jax.experimental.pallas import tpu as pltpu
from jax.sharding import PartitionSpec as P

MESH = pl.DeviceIdType.MESH
BF = jnp.bfloat16
F32 = jnp.float32
STEPS = 4
DEPTH = 512
ORDER = ("q|e", "eq", "eq", "q|e")


def halves(value):
    high = value.astype(BF)
    return high, (value - high.astype(F32)).astype(BF)


def kernel(
    t_ref, b1_ref, b2_ref, b3_ref, e1_ref, e2_ref, e3_ref, noise_ref, o_ref,
    re1, se2, re2, se3, rq1, sq2, rq2, sq3, r3, s3,
    re3p, se2p, re2p, se1p, rq3p, sq2p, rq2p, sq1p,
    b1f, b2f, b3f, b3c, b3tc, b2l, b2tl, b1l, b1tm, lhs, rhs, mid, e1b,
    base_sem, send, in_e1, in_q1, in_e2, in_q2, in_me, in_mq, in_e3p, in_q3p, in_e2p, in_q2p, in_out,
):
    w, x, q = lax.axis_index("gx"), lax.axis_index("gy"), lax.axis_index("gz")
    y, z, core = w // 2, (q // 2) * 2 + w % 2, q % 2
    beta = w * 4 + q

    def far(dy, dz, dc):
        y2, z2, c2 = (y + dy) % 4, (z + dz) % 4, (core + dc) % 2
        return y2 * 2 + z2 % 2, (z2 // 2) * 2 + c2

    def each_far(act):
        def both(n, _):
            k = n // 2
            act(*far(k % 3 + 1, (k % 3 + k // 3) % 3 + 1, n % 2))
            return _

        def one(n, _):
            act(*far(n // 2 + 1, 0, n % 2))
            return _

        def other(n, _):
            act(*far(0, n // 2 + 1, n % 2))
            return _

        lax.fori_loop(0, 18, both, 0)
        lax.fori_loop(0, 6, one, 0)
        lax.fori_loop(0, 6, other, 0)
        act(*far(0, 0, 1))

    def push(src, dst, sem, arrival, where):
        pltpu.make_async_remote_copy(
            src_ref=src, dst_ref=dst, send_sem=send.at[sem], recv_sem=arrival,
            device_id=where, device_id_type=MESH,
        ).start()

    def await_bytes(ref, sem):
        pltpu.make_async_copy(ref, ref, sem).wait()

    def staged(part_e, part_q, orders):
        for order in orders.split("|"):
            def body(s, _):
                for part in order:
                    (part_e if part == "e" else part_q)(s)
                return _

            lax.fori_loop(0, STEPS, body, 0)

    loads = [
        pltpu.make_async_copy(ref, buf, base_sem.at[n])
        for n, (ref, buf) in enumerate(((b3_ref, b3f), (b2_ref, b2f), (b1_ref, b1f)))
    ]
    for load in loads:
        load.start()

    barrier = pltpu.get_barrier_semaphore()

    def greet(w2, q2):
        pl.semaphore_signal(barrier, inc=1, device_id=(w2, x, q2), device_id_type=MESH)

    for d in (1, 2, 3):
        pl.semaphore_signal(barrier, inc=1, device_id=(w, (x + d) % 4, q), device_id_type=MESH)
    each_far(greet)
    pl.semaphore_wait(barrier, 34)

    def first(s, _):
        two = pl.ds(s * 2, 2)
        for d in (2, 1, 3):
            q2, x2 = (q + d) % 4, (x + d) % 4
            push(t_ref.at[pl.ds(q2 * 8 + s * 2, 2)], re1.at[q, two], 0, in_e1.at[s], (w, x, q2))
            push(t_ref.at[pl.ds(32 + x2 * 8 + s * 2, 2)], rq1.at[two, x], 1, in_q1.at[s], (w, x2, q))
        pltpu.make_async_copy(t_ref.at[pl.ds(q * 8 + s * 2, 2)], re1.at[q, two], in_e1.at[s]).start()
        pltpu.make_async_copy(t_ref.at[pl.ds(32 + x * 8 + s * 2, 2)], rq1.at[two, x], in_q1.at[s]).start()
        return _

    lax.fori_loop(0, STEPS, first, 0)

    def columns(target, value):
        high, low = halves(value)
        target[0:512, :] = high
        target[512:1024, :] = low
        target[1024:1536, :] = high

    def rows(target, value):
        high, low = halves(value)
        target[:, 0:512] = high
        target[:, 512:1024] = high
        target[:, 1024:1536] = low

    loads[1].wait()
    rows(b2tl, b2f[...].T)
    loads[0].wait()
    columns(b3c, b3f[...])

    def data_left(piece, factor):
        for k in range(4):
            high, low = halves(piece(k))
            lhs[:, k * 128 : k * 128 + 128] = high
            lhs[:, 512 + k * 128 : 640 + k * 128] = high
            lhs[:, 1024 + k * 128 : 1152 + k * 128] = low
        return jnp.dot(lhs[...], factor[...], preferred_element_type=F32)

    def data_right(factor, piece):
        for k in range(2):
            high, low = halves(piece(k))
            lanes = slice(k * 128, k * 128 + 128)
            rhs[0:512, lanes] = high
            rhs[512:1024, lanes] = low
            rhs[1024:1536, lanes] = high
        return jnp.dot(factor[...], rhs[...], preferred_element_type=F32)

    def stage_one_e(s):
        two = pl.ds(s * 2, 2)
        await_bytes(re1.at[:, two], in_e1.at[s])
        out = data_left(lambda k: re1[k, two].reshape(256, 128), b3c)
        for n in range(4):
            se2[n, two] = out[:, n * 128 : n * 128 + 128].reshape(2, 128, 128)
        for d in (2, 1, 3):
            x2 = (x + d) % 4
            push(se2.at[x2, two], re2.at[two, x], 2, in_e2.at[s], (w, x2, q))
        re2[two, x] = se2[x, two]

    def stage_one_q(s):
        two = pl.ds(s * 2, 2)
        await_bytes(rq1.at[two], in_q1.at[s])
        out = data_right(b2tl, lambda k: rq1[s * 2 + k].reshape(512, 128))
        sq2[s * 2] = out[:, 0:128]
        sq2[s * 2 + 1] = out[:, 128:256]

        def spread(w2, q2):
            push(
                sq2.at[two, pl.ds((w2 * 4 + q2) * 16, 16)], rq2.at[q, w, two],
                3, in_q2.at[s], (w2, x, q2),
            )

        each_far(spread)
        rq2[q, w, two] = sq2[two, pl.ds(pl.multiple_of(beta * 16, 16), 16)]

    staged(stage_one_e, stage_one_q, ORDER[0])

    loads[2].wait()
    place = lax.broadcasted_iota(jnp.int32, (DEPTH, DEPTH), 0)
    source = (place % 128) // 2 * 8 + place // 128 * 2 + place % 2
    pick = (lax.broadcasted_iota(jnp.int32, (DEPTH, DEPTH), 1) == source).astype(F32).astype(BF)
    high, low = halves(b1f[...])
    high = jnp.dot(pick, high, preferred_element_type=F32)
    low = jnp.dot(pick, low, preferred_element_type=F32)
    b1l[:, 0:512] = high.astype(BF)
    b1l[:, 512:1024] = high.astype(BF)
    b1l[:, 1024:1536] = low.astype(BF)
    high, low = high.T.astype(BF), low.T.astype(BF)
    for n in range(STEPS):
        b1tm[n, :, 0:128] = high[:, n * 128 : n * 128 + 128]
        b1tm[n, :, 128:256] = high[:, n * 128 : n * 128 + 128]
        b1tm[n, :, 256:384] = low[:, n * 128 : n * 128 + 128]
    s3[...] = jnp.zeros_like(s3)
    e1b[...] = jnp.broadcast_to(e1_ref[...], (128, DEPTH)).T
    along = e3_ref[pl.ds(x, 1), :]
    inverse = (se1p.reshape(4096, 128), sq1p.reshape(4096, 128))

    def column(at):
        return pl.ds(pl.multiple_of(at * DEPTH, DEPTH), DEPTH)

    def invert(pair, _):
        for k in range(2):
            spectrum = e1b[...] * e2_ref[beta * 16 + pair * 2 + k] * along + noise_ref[0]
            inverse[k][column(pair), :] = 1.0 / spectrum
        return _

    lax.fori_loop(0, 8, invert, 0)

    def stage_two_e(s):
        two = pl.ds(s * 2, 2)
        await_bytes(re2.at[two, pl.ds(0, 3)], in_e2.at[s])
        out = data_right(b2tl, lambda k: re2[s * 2 + k].reshape(512, 128))
        se3[s * 2] = out[:, 0:128]
        se3[s * 2 + 1] = out[:, 128:256]

        def spread(w2, q2):
            push(
                se3.at[two, pl.ds((w2 * 4 + q2) * 16, 16)], r3.at[s, w, 0, q],
                4, in_me.at[s], (w2, x, q2),
            )

        each_far(spread)
        r3[s, w, 0, q] = se3[two, pl.ds(pl.multiple_of(beta * 16, 16), 16)]

    def stage_two_q(s):
        two = pl.ds(s * 2, 2)
        await_bytes(sq2.at[pl.ds(0, 2), pl.ds(0, 496)], in_q2.at[s])
        out = data_left(lambda k: rq2[k, :, two].reshape(256, 128), b3c)
        for n in range(4):
            sq3[n, :, two] = out[:, n * 128 : n * 128 + 128].reshape(8, 2, 16, 128)
        for d in (2, 1, 3):
            x2 = (x + d) % 4
            push(sq3.at[x2, :, two], r3.at[s, :, 1, x], 5, in_mq.at[s], (w, x2, q))
        r3[s, :, 1, x] = sq3[x, :, two]

    staged(stage_two_e, stage_two_q, ORDER[1])

    rows(b2l, b2f[...])
    columns(b3tc, b3f[...].T)

    flat = r3.reshape(8192, 128)
    flat_s = s3.reshape(8192, 128)
    def arrived(s):
        await_bytes(se3.at[pl.ds(0, 2), pl.ds(0, 496)], in_me.at[s])
        await_bytes(sq3.at[pl.ds(0, 3), :, pl.ds(0, 2)], in_mq.at[s])

    def term(s, pair):
        for k in range(2):
            high, low = halves(flat[pl.ds(s * 2048 + pair * 2 + k, 128, stride=16), :])
            lanes = slice(k * 128, k * 128 + 128)
            rhs[0:128, lanes] = high
            rhs[128:256, lanes] = low
            rhs[256:384, lanes] = high
        return jnp.dot(b1tm[s], rhs[0:384, :], preferred_element_type=F32)

    def total(at):
        return flat_s.at[column(at), :]

    def gather_sum(s, _):
        arrived(s)

        def one_pair(pair, _):
            part = term(s, pair)
            for k in range(2):
                total(pair * 2 + k)[...] += part[:, k * 128 : k * 128 + 128]
            return _

        lax.fori_loop(0, 8, one_pair, 0)
        return _

    lax.fori_loop(0, STEPS - 1, gather_sum, 0)
    arrived(STEPS - 1)

    def middle(pair, _):
        part = term(STEPS - 1, pair)
        for k in range(2):
            at = pair * 2 + k
            lanes = slice(k * 128, k * 128 + 128)
            high, low = halves((total(at)[...] + part[:, lanes]) * inverse[k][column(pair), :])
            mid[pair, 0:512, lanes] = high
            mid[pair, 512:1024, lanes] = low
        return _

    def turn(s, pair):
        factor = b1l[pl.ds(pl.multiple_of(s * 128, 128), 128), :]
        out = jnp.dot(factor[:, 0:1024], mid[pair], preferred_element_type=F32)
        out += jnp.dot(factor[:, 1024:1536], mid[pair, 0:512], preferred_element_type=F32)
        for k in range(2):
            flat_s[pl.ds(s * 2048 + pair * 2 + k, 128, stride=16), :] = out[:, k * 128 : k * 128 + 128]

    def send_back(s, low, count):
        some = pl.ds(low, count)
        mine = pl.ds(pl.multiple_of(beta * 16 + low, 8), count)
        two = pl.ds(s * 2, 2)
        for d in (2, 1, 3):
            x2 = (x + d) % 4
            push(s3.at[s, :, 1, x2, :, some], rq3p.at[x, s, :, :, some], 6, in_q3p.at[s], (w, x2, q))

        def spread(w2, q2):
            push(s3.at[s, w2, 0, q2, :, some], re3p.at[two, mine], 7, in_e3p.at[s], (w2, x, q2))

        each_far(spread)
        rq3p[x, s, :, :, some] = s3[s, :, 1, x, :, some]
        re3p[two, mine] = s3[s, w, 0, q, :, some]

    for part in range(2):
        lax.fori_loop(part * 4, part * 4 + 4, middle, 0)
        for pair in range(part * 4, part * 4 + 4):
            turn(0, pair)
        send_back(0, part * 8, 8)

    def back_mid(s, _):
        for pair in range(8):
            turn(s, pair)
        send_back(s, 0, 16)
        return _

    lax.fori_loop(1, STEPS, back_mid, 0)

    def back_one_e(s):
        two = pl.ds(s * 2, 2)
        await_bytes(se3.at[pl.ds(0, 2), pl.ds(0, 496)], in_e3p.at[s])
        out = data_right(b2l, lambda k: re3p[s * 2 + k])
        for k in range(2):
            se2p[s * 2 + k] = out[:, k * 128 : k * 128 + 128].reshape(4, 128, 128)
        for d in (2, 1, 3):
            x2 = (x + d) % 4
            push(se2p.at[two, x2], re2p.at[x, two], 9, in_e2p.at[s], (w, x2, q))
        re2p[x, two] = se2p[two, x]

    def back_one_q(s):
        two = pl.ds(s * 2, 2)
        await_bytes(rq3p.at[pl.ds(0, 3), s], in_q3p.at[s])
        out = data_left(lambda k: rq3p[k, s].reshape(256, 128), b3tc)
        for n in range(4):
            sq2p[n, s] = out[:, n * 128 : n * 128 + 128].reshape(8, 2, 16, 128)

        def spread(w2, q2):
            push(
                sq2p.at[q2, s, w2],
                rq2p.at[two, pl.ds(pl.multiple_of(beta * 16, 16), 16)],
                8, in_q2p.at[s], (w2, x, q2),
            )

        each_far(spread)
        rq2p[two, pl.ds(pl.multiple_of(beta * 16, 16), 16)] = sq2p[q, s, w]

    staged(back_one_e, back_one_q, ORDER[2])

    def back_two_e(s):
        two = pl.ds(s * 2, 2)
        await_bytes(re2p.at[pl.ds(0, 3), two], in_e2p.at[s])
        out = data_left(lambda k: re2p[k, two].reshape(256, 128), b3tc)
        for n in range(4):
            se1p[n, two] = out[:, n * 128 : n * 128 + 128].reshape(2, 128, 128)
        here = o_ref.at[pl.ds(q * 8 + s * 2, 2)]
        for d in (2, 1, 3):
            q2 = (q + d) % 4
            push(se1p.at[q2, two], here, 10, in_out.at[0], (w, x, q2))
        pltpu.make_async_copy(se1p.at[q, two], here, in_out.at[0]).start()

    def back_two_q(s):
        two = pl.ds(s * 2, 2)
        await_bytes(se3.at[pl.ds(0, 2), pl.ds(0, 496)], in_q2p.at[s])
        out = data_right(b2l, lambda k: rq2p[s * 2 + k])
        for k in range(2):
            sq1p[s * 2 + k] = out[:, k * 128 : k * 128 + 128].reshape(4, 128, 128)
        here = o_ref.at[pl.ds(32 + x * 8 + s * 2, 2)]
        for d in (2, 1, 3):
            x2 = (x + d) % 4
            push(sq1p.at[two, x2], here, 11, in_out.at[1], (w, x2, q))
        pltpu.make_async_copy(sq1p.at[two, x], here, in_out.at[1]).start()

    staged(back_two_e, back_two_q, ORDER[3])

    await_bytes(re1, in_out.at[0])
    await_bytes(re1, in_out.at[1])
    for sem in (0, 1, 2, 5, 6, 9, 10, 11):
        await_bytes(re1.at[pl.ds(0, 3)], send.at[sem])
    for sem in (3, 4, 7, 8):
        await_bytes(se3.at[:, pl.ds(0, 496)], send.at[sem])


def per_device(targets, basis_first, basis_second, basis_third, eigen_first, eigen_second, eigen_third, noise):
    half = [
        (4, 8, 128, 128), (4, 8, 128, 128), (8, 4, 128, 128), (8, 512, 128),
        (8, 4, 128, 128), (8, 512, 128), (4, 8, 8, 16, 128), (4, 8, 8, 16, 128),
        (4, 8, 2, 4, 2, 16, 128), (4, 8, 2, 4, 2, 16, 128),
        (8, 512, 128), (8, 4, 128, 128), (4, 8, 128, 128), (4, 8, 128, 128),
        (4, 4, 8, 2, 16, 128), (4, 4, 8, 2, 16, 128), (8, 512, 128), (8, 4, 128, 128),
    ]
    scratch = [pltpu.VMEM(shape, F32) for shape in half]
    scratch += [pltpu.VMEM((512, 512), F32)] * 3
    scratch += [pltpu.VMEM((1536, 512), BF)] * 2 + [pltpu.VMEM((512, 1536), BF)] * 3 + [pltpu.VMEM((4, 512, 384), BF)]
    scratch += [pltpu.VMEM((256, 1536), BF), pltpu.VMEM((1536, 256), BF)]
    scratch += [pltpu.VMEM((8, 1024, 256), BF), pltpu.VMEM((512, 128), F32)]
    dma = pltpu.SemaphoreType.DMA
    scratch += [dma((3,)), dma((12,))] + [dma((STEPS,))] * 4
    scratch += [dma((STEPS,))] * 6 + [dma((2,))]
    whole = pl.BlockSpec(memory_space=pl.ANY)
    vmem = pl.BlockSpec(memory_space=pltpu.VMEM)
    smem = pl.BlockSpec(memory_space=pltpu.SMEM)
    return pl.pallas_call(
        kernel,
        out_shape=pltpu.VMEM((64, 128, 128), F32),
        in_specs=[whole, whole, whole, whole, vmem, smem, vmem, smem],
        out_specs=vmem,
        scratch_shapes=scratch,
        compiler_params=pltpu.CompilerParams(
            collective_id=0, has_side_effects=True, vmem_limit_bytes=62500000
        ),
        name="kron_solve",
    )(
        targets, basis_first, basis_second, basis_third,
        eigen_first.reshape(1, 512), eigen_second, eigen_third.reshape(4, 128), noise,
    )


def solution(mesh):
    in_specs = (P("gx", "gy", "gz"), P(), P(), P(), P(), P(), P(), P())
    return jax.shard_map(
        per_device, mesh=mesh, in_specs=in_specs, out_specs=P("gx", "gy", "gz"), check_vma=False
    )
```
